32 devices in a mesh: depth: 16 (over z, y, x), chan: 2 (over core).
Axes of the slice: x: 2, y: 2, z: 4, core: 2. Of those that a mesh axis runs over, the one named last changes fastest.
Arguments:
- feats: bfloat16 [32, 32, 8, 128], P('chan', 'depth'), may hold values from -6 to 6
- weight_one: bfloat16 [32, 32, 27], replicated, may hold values from -0.21875 to 0.21875
- weight_two: bfloat16 [64, 32, 27], replicated, may hold values from -0.21875 to 0.21875
- cotangent: bfloat16 [64, 16, 4, 64], P('chan', 'depth'), may hold values from -6 to 6
Outputs:
- grad_feats: bfloat16 [32, 32, 8, 128], P('chan', 'depth')
- grad_weight_one: float32 [32, 32, 27], P(None, 'chan')
- grad_weight_two: float32 [64, 32, 27], P(None, 'chan')
The draws below stay inside these ranges and needn't reach their ends.
All inputs are finite; a program needn't handle non-finite values.
Results may differ from the reference program's by a relative error of at most 0.013.
Values may be sent and summed in bfloat16 or wider, within the bound.
A program may use at most 128 MiB of HBM per device.

```python
import jax
import jax.numpy as jnp
from jax import lax

C0 = 32
C1 = 64
H = 8
W = 128
NZ = 32


def shard_levels(rng, dims, cuts, low, largest):
    factor_of, own = 1.0, jax.random.fold_in(rng, 6)
    for axis_at, blocks in cuts:
        draws = jnp.exp(jax.random.uniform(jax.random.fold_in(own, axis_at), (blocks,), jnp.float32, low / len(cuts), largest / len(cuts)))
        factor_of = factor_of * jnp.repeat(draws, dims[axis_at] // blocks).reshape([-1 if axis == axis_at else 1 for axis in range(len(dims))])
    return factor_of


def gaussian(rng, shape, scale, bound, cuts=(), held_as=jnp.bfloat16):
    entries = scale * jax.random.normal(rng, shape, jnp.float32)
    if cuts:
        entries = entries * shard_levels(rng, shape, cuts, -0.22, 0.18)
    return jnp.clip(entries, -bound, bound).astype(held_as)


def setup_inputs(seed: int = 0) -> dict:
    splits = jax.random.split(jax.random.key(seed), 5)
    feats = gaussian(splits[0], (C0, NZ, H, W), 1.0, 6.0, ((0, 2), (1, 16)))
    weight_one = gaussian(splits[1], (C0, C0, 27), (27 * C0) ** -0.5, 0.21875)
    weight_two = gaussian(splits[2], (C1, C0, 27), (27 * C0) ** -0.5, 0.21875)
    cotangent = gaussian(splits[3], (C1, NZ // 2, H // 2, W // 2), 1.0, 6.0, ((0, 2), (1, 16)))
    return dict(feats=feats, weight_one=weight_one, weight_two=weight_two, cotangent=cotangent)


OFFSETS = [(first, second, third) for first in range(3) for second in range(3) for third in range(3)]

def pad_all(field):
    return jnp.pad(field.astype(jnp.float32), ((0, 0), (1, 1), (1, 1), (1, 1)))

def convolve(field, weight):
    chans, planes, height, across = field.shape
    padded = pad_all(field)
    total = jnp.zeros((weight.shape[0], planes, height, across), jnp.float32)
    for index, (first, second, third) in enumerate(OFFSETS):
        window = padded[:, first:first + planes, second:second + height, third:third + across]
        total = total + jnp.einsum('oi,izhw->ozhw', weight[:, :, index].astype(jnp.float32), window, precision=lax.Precision.HIGHEST)
    return total

def transpose_conv(grads, weight):
    chans, planes, height, across = grads.shape
    padded = pad_all(grads)
    total = jnp.zeros((weight.shape[1], planes, height, across), jnp.float32)
    for index, (first, second, third) in enumerate(OFFSETS):
        window = padded[:, 2 - first:2 - first + planes, 2 - second:2 - second + height, 2 - third:2 - third + across]
        total = total + jnp.einsum('oi,ozhw->izhw', weight[:, :, index].astype(jnp.float32), window, precision=lax.Precision.HIGHEST)
    return total

def weight_grad(grads, field):
    chans, planes, height, across = field.shape
    padded = pad_all(field)
    grads_wide = grads.astype(jnp.float32)
    pieces = []
    for index, (first, second, third) in enumerate(OFFSETS):
        window = padded[:, first:first + planes, second:second + height, third:third + across]
        pieces.append(jnp.einsum('ozhw,izhw->oi', grads_wide, window, precision=lax.Precision.HIGHEST))
    return jnp.stack(pieces, axis=-1)

def slope(pre):
    sig = jax.nn.sigmoid(pre)
    return sig * (1.0 + pre * (1.0 - sig))

def one_volume(feats, weight_one, weight_two, cotangent):
    chans, planes, height, across = feats.shape
    pre_one = convolve(feats, weight_one)
    act_one = jax.nn.silu(pre_one).astype(jnp.bfloat16)
    pooled = act_one.astype(jnp.float32).reshape(chans, planes // 2, 2, height // 2, 2, across // 2, 2).mean(axis=(2, 4, 6)).astype(jnp.bfloat16)
    pre_two = convolve(pooled, weight_two)
    grad_two = (cotangent.astype(jnp.float32) * slope(pre_two)).astype(jnp.bfloat16)
    grad_weight_two = weight_grad(grad_two, pooled)
    back_pooled = transpose_conv(grad_two, weight_two)
    spread = jnp.repeat(jnp.repeat(jnp.repeat(back_pooled, 2, axis=1), 2, axis=2), 2, axis=3) * 0.125
    grad_one = (spread * slope(pre_one)).astype(jnp.bfloat16)
    grad_weight_one = weight_grad(grad_one, feats)
    grad_feats = transpose_conv(grad_one, weight_one).astype(jnp.bfloat16)
    return (grad_feats, grad_weight_one, grad_weight_two)

def reference(feats, weight_one, weight_two, cotangent):
    return one_volume(feats, weight_one, weight_two, cotangent)
```

```python
import functools

import jax
import jax.numpy as jnp
from jax import lax
from jax.experimental import pallas as pl
from jax.experimental.pallas import tpu as pltpu
from jax.sharding import PartitionSpec as P

MESH = pl.DeviceIdType.MESH
BF16 = jnp.bfloat16
F32 = jnp.float32


def dot(left, right):
    return jnp.dot(left, right, preferred_element_type=F32)


def dot_nt(left, right):
    return lax.dot_general(left, right, (((1,), (1,)), ((), ())), preferred_element_type=F32)


def slope(pre):
    sig = jax.nn.sigmoid(pre)
    return sig * (1.0 + pre * (1.0 - sig))


def plane_taps(field, across):
    chans, cells = field.shape
    wide = field.astype(F32)
    cell = lax.broadcasted_iota(jnp.int32, (chans, cells), 1)
    column = lax.rem(cell, across)
    moved = [
        jnp.where(column == 0, 0.0, pltpu.roll(wide, 1, 1)),
        wide,
        jnp.where(column == across - 1, 0.0, pltpu.roll(wide, cells - 1, 1)),
    ]
    if across % 128 == 0:
        moved = [m.astype(BF16) for m in moved]
        edge = jnp.zeros((chans, across), BF16)
        above = [jnp.concatenate([edge, m[:, :-across]], axis=1) for m in moved]
        below = [jnp.concatenate([m[:, across:], edge], axis=1) for m in moved]
        return above + moved + below
    above = [jnp.where(cell < across, 0.0, pltpu.roll(m, across, 1)) for m in moved]
    below = [
        jnp.where(cell >= cells - across, 0.0, pltpu.roll(m, cells - across, 1)) for m in moved
    ]
    return [m.astype(BF16) for m in above + moved + below]


def kernel(
    n, owners, across,
    feats, cot, w1f, w1b, w2f, w2b,
    out_feats, out_one, out_two,
    halo, cots, pools, x1, x2, xg1, xg2, slopes, shrink, spread,
    part1, land1, full1, part2, land2, full2,
    send_f, recv_f, send_c, recv_c, send_p, recv_p,
    send_r1, recv_r1, send_a1, recv_a1, send_r2, recv_r2, send_a2, recv_a2,
):
    place = lax.axis_index("depth")
    core = lax.axis_index("chan")
    other = 1 - core
    half = feats.shape[1]
    cells = feats.shape[2]
    small = cot.shape[1]
    rows1 = 9 * half
    stride = n // owners

    def at(step):
        return lax.rem(place + step + n, n)

    barrier = pltpu.get_barrier_semaphore()

    def greet(device):
        pl.semaphore_signal(barrier, inc=1, device_id=device, device_id_type=MESH)

    greet((place, other))
    for step in (1, -1, 2, -2):
        greet((at(step), other))

    def greet_row(step, carry):
        greet((at(step), core))
        return carry

    lax.fori_loop(1, n, greet_row, 0)

    def valid(step):
        return jnp.logical_and(place + step >= 0, place + step < n)

    def put_x1(plane, side, field):
        for tap, block in enumerate(plane_taps(field, across)):
            x1[side, pl.ds(plane * rows1 + tap * half, half), :] = block

    big_row = lax.broadcasted_iota(jnp.int32, (cells, small), 0)
    small_col = lax.broadcasted_iota(jnp.int32, (cells, small), 1)
    target = (big_row // (2 * across)) * (across // 2) + lax.rem(big_row, across) // 2
    shrink[...] = jnp.where(target == small_col, 0.125, 0.0).astype(BF16)
    big_col = lax.broadcasted_iota(jnp.int32, (small, cells), 1)
    small_row = lax.broadcasted_iota(jnp.int32, (small, cells), 0)
    target = (big_col // (2 * across)) * (across // 2) + lax.rem(big_col, across) // 2
    spread[...] = jnp.where(target == small_row, 0.125, 0.0).astype(BF16)

    for plane in range(2):
        put_x1(2 + plane, core, feats[plane])
    cots[2, core] = cot[...]

    pl.semaphore_wait(barrier, n + 4)

    def copy(src, dst, send, recv, device):
        return pltpu.make_async_remote_copy(
            src_ref=src, dst_ref=dst, send_sem=send, recv_sem=recv,
            device_id=device, device_id_type=MESH,
        )

    near, far = [], []
    mate = copy(feats, halo.at[pl.ds(2, 2), core], send_f.at[0], recv_f.at[0], (place, other))
    mate.start()
    index = 1
    for planes in ((1, 0), (0, 1)):
        for step, plane in zip((1, -1), planes):
            for who in (core, other):
                to = plane if step == 1 else 4 + plane
                one = copy(
                    feats.at[plane], halo.at[to, core], send_f.at[index], recv_f.at[index],
                    (at(step), who),
                )
                one.start()
                (near if index < 5 else far).append(one)
                index += 1
    cot_copies = []
    index = 0
    targets = [(0, other)] + [(s, w) for s in (1, -1, 2, -2) for w in (core, other)]
    for step, who in targets:
        one = copy(
            cot, cots.at[2 - step, core], send_c.at[index], recv_c.at[index], (at(step), who)
        )
        one.start()
        cot_copies.append(one)
        index += 1

    def take_halo(plane, side, keep):
        field = halo[plane, side]
        if keep is not None:
            field = jnp.where(keep, field.astype(F32), 0.0)
        put_x1(plane, side, field)

    def conv_one(plane):
        total = dot(w1f[0], x1[0, (plane - 1) * rows1 : (plane + 2) * rows1, :])
        return total + dot(w1f[1], x1[1, (plane - 1) * rows1 : (plane + 2) * rows1, :])

    mate.wait_recv()
    for plane in (2, 3):
        take_halo(plane, other, None)
    for one in near:
        one.wait_recv()
    for plane, step in ((1, -1), (4, 1)):
        for side in range(2):
            take_halo(plane, side, valid(step))

    pooled = None
    for plane in (2, 3):
        pre = conv_one(plane)
        sig = jax.nn.sigmoid(pre)
        slopes[plane - 1] = sig * (1.0 + pre * (1.0 - sig))
        term = dot((pre * sig).astype(BF16), shrink[...])
        pooled = term if pooled is None else pooled + term
    pools[3] = pooled.astype(BF16)
    pool_copies = []
    for index, step in enumerate((1, -1, 2, -2, 3, -3)):
        one = copy(
            pools.at[3], pools.at[3 - step], send_p.at[index], recv_p.at[index], (at(step), core)
        )
        one.start()
        pool_copies.append(one)

    for one in far:
        one.wait_recv()
    for plane, step in ((0, -1), (5, 1)):
        for side in range(2):
            take_halo(plane, side, valid(step))
    for plane in (1, 4):
        slopes[plane - 1] = slope(conv_one(plane))

    def put_x2(plane, keep):
        field = pools[plane].astype(F32)
        if keep is not None:
            field = jnp.where(keep, field, 0.0)
        for tap, block in enumerate(plane_taps(field, across // 2)):
            for side in range(2):
                x2[side, pl.ds(plane * rows1 + tap * half, half), :] = block[
                    side * half : (side + 1) * half
                ]

    put_x2(3, None)
    for one in cot_copies:
        one.wait_recv()
    for one in pool_copies:
        one.wait_recv()
    for plane in (2, 4, 1, 5, 0, 6):
        put_x2(plane, valid(plane - 3))

    outs = 2 * cot.shape[0]
    rows2 = 9 * outs
    own_grad = None
    for plane in range(5):
        pre = dot(w2f[0], x2[0, plane * rows1 : (plane + 3) * rows1, :])
        pre = pre + dot(w2f[1], x2[1, plane * rows1 : (plane + 3) * rows1, :])
        grad = cots[plane].reshape(outs, small).astype(F32) * slope(pre)
        if plane != 2:
            grad = jnp.where(valid(plane - 2), grad, 0.0)
        else:
            own_grad = grad.astype(BF16)
        grad = grad.astype(BF16)
        for tap, block in enumerate(plane_taps(grad, across // 2)):
            xg2[pl.ds(plane * rows2 + tap * outs, outs), :] = block

    lanes = 512
    mine = place // stride
    is_owner = lax.rem(place, stride) == 0

    def when_owner(body):
        if stride == 1:
            body()
        else:
            pl.when(is_owner)(body)

    def chunk_out(total, part):
        rows = part.shape[1]
        for chunk in range(owners):
            r, l = chunk // 4, chunk % 4
            part[chunk] = total[r * rows : (r + 1) * rows, l * 128 : (l + 1) * 128].astype(BF16)

    def scatter_copy(part, land, send, recv, chunk, source, device):
        return copy(part.at[chunk], land.at[source], send.at[chunk], recv.at[source], device)

    def scatter(part, land, send, recv):
        def go(step, carry):
            chunk = lax.rem(mine + step, owners)

            @pl.when(chunk * stride != place)
            def _():
                scatter_copy(part, land, send, recv, chunk, place, (chunk * stride, core)).start()

            return carry

        lax.fori_loop(0, owners, go, 0)

        @when_owner
        def _():
            land[place] = part[mine]

    def gather(part, land, full, recv_r, send, recv):
        @when_owner
        def _():
            def arrived(step, carry):
                source = at(step)
                scatter_copy(part, land, send, recv_r, 0, source, (place, other)).wait_recv()
                return carry

            lax.fori_loop(1, n, arrived, 0)
            full[mine] = jnp.sum(land[...].astype(F32), axis=0).astype(BF16)

            def go(step, carry):
                copy(
                    full.at[mine], full.at[mine], send.at[at(step)], recv.at[mine], (at(step), core)
                ).start()
                return carry

            lax.fori_loop(1, n, go, 0)

    def finish(part, land, full, send_r, send, recv, out):
        def came(chunk, carry):
            @pl.when(chunk * stride != place)
            def _():
                copy(
                    full.at[chunk], full.at[chunk], send.at[0], recv.at[chunk], (place, other)
                ).wait_recv()
                scatter_copy(part, land, send_r, recv, chunk, 0, (place, other)).wait_send()

            return carry

        lax.fori_loop(0, owners, came, 0)

        @when_owner
        def _():
            def sent(step, carry):
                copy(
                    full.at[mine], full.at[mine], send.at[at(step)], recv.at[0], (place, other)
                ).wait_send()
                return carry

            lax.fori_loop(1, n, sent, 0)

        rows = part.shape[1]
        for chunk in range(owners):
            r, l = chunk // 4, chunk % 4
            out[r * rows : (r + 1) * rows, l * 128 : (l + 1) * 128] = full[chunk].astype(F32)

    total2 = dot_nt(own_grad, x2[core, 2 * rows1 : 2 * rows1 + lanes, :])
    chunk_out(total2, part2)
    scatter(part2, land2, send_r2, recv_r2)

    grads = []
    for plane in range(3):
        back = dot(w2b[...], xg2[plane * rows2 : (plane + 3) * rows2, :]).astype(BF16)
        wide = dot(back, spread[...])
        for where in ((0,), (1, 2), (3,))[plane]:
            grad = wide * slopes[where]
            if plane != 1:
                grad = jnp.where(valid(plane - 1), grad, 0.0)
            grads.append(grad.astype(BF16))

    total1 = dot_nt(grads[1], x1[core, rows1 : rows1 + lanes, :])
    total1 = total1 + dot_nt(grads[2], x1[core, 2 * rows1 : 2 * rows1 + lanes, :])
    chunk_out(total1, part1)
    scatter(part1, land1, send_r1, recv_r1)
    gather(part2, land2, full2, recv_r2, send_a2, recv_a2)

    mids = 2 * half
    rows_g = 9 * mids
    for plane in range(4):
        for tap, block in enumerate(plane_taps(grads[plane], across)):
            xg1[pl.ds(plane * rows_g + tap * mids, mids), :] = block
    for plane in range(2):
        out_feats[plane] = dot(w1b[core], xg1[plane * rows_g : (plane + 3) * rows_g, :]).astype(BF16)

    gather(part1, land1, full1, recv_r1, send_a1, recv_a1)
    for one in [mate] + near + far + cot_copies + pool_copies:
        one.wait_send()
    finish(part2, land2, full2, send_r2, send_a2, recv_a2, out_two)
    finish(part1, land1, full1, send_r1, send_a1, recv_a1, out_one)


def shards(feats, weight_one, weight_two, cotangent):
    n = lax.axis_size("depth")
    owners = 16
    half, planes, height, across = feats.shape
    cells = height * across
    mids = weight_one.shape[0]
    outs = weight_two.shape[0]
    small = cells // 4
    x = jnp.transpose(feats.reshape(half, planes, cells), (1, 0, 2))
    cot = cotangent.reshape(outs // 2, small)

    def forward(weight):
        o = weight.shape[0]
        return jnp.transpose(weight.reshape(o, 2, half, 27), (1, 0, 3, 2)).reshape(2, o, 27 * half)

    def backward(weight):
        return jnp.transpose(weight[:, :, ::-1], (1, 2, 0)).reshape(weight.shape[1], -1)

    w1f, w2f = forward(weight_one), forward(weight_two)
    w1b = backward(weight_one).reshape(2, half, 27 * mids)
    w2b = backward(weight_two)
    vmem = pl.BlockSpec(memory_space=pltpu.VMEM)
    dma = pltpu.SemaphoreType.DMA
    out_feats, out_one, out_two = pl.pallas_call(
        functools.partial(kernel, n, owners, across),
        out_shape=(
            jax.ShapeDtypeStruct((planes, half, cells), BF16),
            jax.ShapeDtypeStruct((mids, 512), F32),
            jax.ShapeDtypeStruct((outs, 512), F32),
        ),
        in_specs=[vmem] * 6,
        out_specs=(vmem,) * 3,
        scratch_shapes=[
            pltpu.VMEM((6, 2, half, cells), BF16),
            pltpu.VMEM((5, 2, outs // 2, small), BF16),
            pltpu.VMEM((7, mids, small), BF16),
            pltpu.VMEM((2, 6 * 9 * half, cells), BF16),
            pltpu.VMEM((2, 7 * 9 * half, small), BF16),
            pltpu.VMEM((4 * 9 * mids, cells), BF16),
            pltpu.VMEM((5 * 9 * outs, small), BF16),
            pltpu.VMEM((4, mids, cells), F32),
            pltpu.VMEM((cells, small), BF16),
            pltpu.VMEM((small, cells), BF16),
            pltpu.VMEM((owners, mids // 4, 128), BF16),
            pltpu.VMEM((n, mids // 4, 128), BF16),
            pltpu.VMEM((owners, mids // 4, 128), BF16),
            pltpu.VMEM((owners, outs // 4, 128), BF16),
            pltpu.VMEM((n, outs // 4, 128), BF16),
            pltpu.VMEM((owners, outs // 4, 128), BF16),
            dma((9,)), dma((9,)), dma((9,)), dma((9,)), dma((6,)), dma((6,)),
            dma((owners,)), dma((n,)), dma((n,)), dma((owners,)),
            dma((owners,)), dma((n,)), dma((n,)), dma((owners,)),
        ],
        compiler_params=pltpu.CompilerParams(
            collective_id=0, has_side_effects=True, vmem_limit_bytes=60 * 1024 * 1024
        ),
    )(x, cot, w1f, w1b, w2f, w2b)

    def layout(total):
        rows = total.shape[0]
        return jnp.transpose(total[:, : 27 * half].reshape(rows, 27, half), (0, 2, 1))

    grad_feats = jnp.transpose(out_feats, (1, 0, 2)).reshape(half, planes, height, across)
    return grad_feats, layout(out_one), layout(out_two)


def solution(mesh):
    return jax.shard_map(
        shards,
        mesh=mesh,
        in_specs=(P("chan", "depth", None, None), P(), P(), P("chan", "depth", None, None)),
        out_specs=(P("chan", "depth", None, None), P(None, "chan", None), P(None, "chan", None)),
        check_vma=False,
    )
```

```python
import functools

import jax
import jax.numpy as jnp
from jax import lax
from jax.experimental import pallas as pl
from jax.experimental.pallas import tpu as pltpu
from jax.sharding import PartitionSpec as P

MESH = pl.DeviceIdType.MESH
BF16 = jnp.bfloat16
F32 = jnp.float32


def dot(left, right):
    return jnp.dot(left, right, preferred_element_type=F32)


def dot_nt(left, right):
    return lax.dot_general(left, right, (((1,), (1,)), ((), ())), preferred_element_type=F32)


def slope(pre):
    sig = jax.nn.sigmoid(pre)
    return sig * (1.0 + pre * (1.0 - sig))


def plane_taps(field, across):
    chans, cells = field.shape
    wide = field.astype(F32)
    cell = lax.broadcasted_iota(jnp.int32, (chans, cells), 1)
    column = lax.rem(cell, across)
    moved = [
        jnp.where(column == 0, 0.0, pltpu.roll(wide, 1, 1)),
        wide,
        jnp.where(column == across - 1, 0.0, pltpu.roll(wide, cells - 1, 1)),
    ]
    if across % 128 == 0:
        moved = [m.astype(BF16) for m in moved]
        edge = jnp.zeros((chans, across), BF16)
        above = [jnp.concatenate([edge, m[:, :-across]], axis=1) for m in moved]
        below = [jnp.concatenate([m[:, across:], edge], axis=1) for m in moved]
        return above + moved + below
    above = [jnp.where(cell < across, 0.0, pltpu.roll(m, across, 1)) for m in moved]
    below = [
        jnp.where(cell >= cells - across, 0.0, pltpu.roll(m, cells - across, 1)) for m in moved
    ]
    return [m.astype(BF16) for m in above + moved + below]


def kernel(
    n, owners, across,
    feats_in, cot_in, w1, w2,
    out_feats, out_one, out_two,
    feats, rel, cot, crel, w1f, w1b, w2f, w2b, halo, cots, pools, x1, x2, xg1, xg2, slopes, shrink, spread,
    part1, land1, full1, part2, land2, full2,
    send_f, recv_f, send_c, recv_c, send_p, recv_p,
    send_r1, recv_r1, send_a1, recv_a1, send_r2, recv_r2, send_a2, recv_a2,
):
    place = lax.axis_index("depth")
    core = lax.axis_index("chan")
    other = 1 - core
    half = feats.shape[1]
    cells = feats.shape[2]
    small = cot.shape[1]
    rows1 = 9 * half
    stride = n // owners

    def at(step):
        return lax.rem(place + step + n, n)

    barrier = pltpu.get_barrier_semaphore()

    def greet(device):
        pl.semaphore_signal(barrier, inc=1, device_id=device, device_id_type=MESH)

    greet((place, other))
    for step in (1, -1, 2, -2):
        greet((at(step), other))

    def greet_row(step, carry):
        greet((at(step), core))
        return carry

    lax.fori_loop(1, n, greet_row, 0)

    def valid(step):
        return jnp.logical_and(place + step >= 0, place + step < n)

    def put_x1(plane, side, field):
        for tap, block in enumerate(plane_taps(field, across)):
            x1[side, pl.ds(plane * rows1 + tap * half, half), :] = block

    big_row = lax.broadcasted_iota(jnp.int32, (cells, small), 0)
    small_col = lax.broadcasted_iota(jnp.int32, (cells, small), 1)
    target = (big_row // (2 * across)) * (across // 2) + lax.rem(big_row, across) // 2
    shrink[...] = jnp.where(target == small_col, 0.125, 0.0).astype(BF16)
    big_col = lax.broadcasted_iota(jnp.int32, (small, cells), 1)
    small_row = lax.broadcasted_iota(jnp.int32, (small, cells), 0)
    target = (big_col // (2 * across)) * (across // 2) + lax.rem(big_col, across) // 2
    spread[...] = jnp.where(target == small_row, 0.125, 0.0).astype(BF16)

    rows = cells // across
    for plane in range(2):
        rel[plane] = feats_in[:, plane].astype(F32).reshape(half * rows, across)
        for row in range(rows):
            feats[plane, :, row * across : (row + 1) * across] = rel[
                plane, pl.ds(row, half, stride=rows), :
            ].astype(BF16)
        put_x1(2 + plane, core, feats[plane])
    short = small // (across // 2)
    for chan in range(cot.shape[0]):
        crel[chan * 8 : chan * 8 + short, :] = cot_in[chan, 0].astype(F32)
    lines = [crel[pl.ds(row, cot.shape[0], stride=8), :] for row in range(short)]
    cot[...] = jnp.concatenate(lines, axis=1).astype(BF16)
    cots[2, core] = cot[...]

    taps, mids, _ = w1.shape
    outs = w2.shape[2]
    for side in range(2):
        lo, hi = side * half, (side + 1) * half
        for tap in range(taps):
            w1f[side, :, tap * half : (tap + 1) * half] = w1[tap][:, lo:hi]
        w2f[side] = w2[:, lo:hi, :].reshape(taps * half, outs).T
    w1b[...] = w1[...].reshape(taps * mids, mids).T.reshape(2, half, taps * mids)
    for tap in range(taps):
        w2b[:, tap * outs : (tap + 1) * outs] = w2[tap]

    pl.semaphore_wait(barrier, n + 4)

    def copy(src, dst, send, recv, device):
        return pltpu.make_async_remote_copy(
            src_ref=src, dst_ref=dst, send_sem=send, recv_sem=recv,
            device_id=device, device_id_type=MESH,
        )

    def launch(one, step):
        pl.when(valid(step))(lambda: one.start())

    def arrive(pairs):
        for one, step in pairs:
            pl.when(valid(-step))(lambda one=one: one.wait_recv())

    def leave(pairs):
        for one, step in pairs:
            pl.when(valid(step))(lambda one=one: one.wait_send())

    near, far = [], []
    mate = copy(feats, halo.at[pl.ds(2, 2), core], send_f.at[0], recv_f.at[0], (place, other))
    mate.start()
    index = 1
    for planes in ((1, 0), (0, 1)):
        for step, plane in zip((1, -1), planes):
            for who in (core, other):
                to = plane if step == 1 else 4 + plane
                one = copy(
                    feats.at[plane], halo.at[to, core], send_f.at[index], recv_f.at[index],
                    (at(step), who),
                )
                launch(one, step)
                (near if index < 5 else far).append((one, step))
                index += 1
    cot_copies = []
    index = 0
    targets = [(0, other)] + [(s, w) for s in (1, -1, 2, -2) for w in (core, other)]
    for step, who in targets:
        one = copy(
            cot, cots.at[2 - step, core], send_c.at[index], recv_c.at[index], (at(step), who)
        )
        launch(one, step)
        cot_copies.append((one, step))
        index += 1

    def take_halo(plane, side, keep):
        field = halo[plane, side]
        if keep is not None:
            field = jnp.where(keep, field.astype(F32), 0.0)
        put_x1(plane, side, field)

    def conv_one(plane):
        total = dot(w1f[0], x1[0, (plane - 1) * rows1 : (plane + 2) * rows1, :])
        return total + dot(w1f[1], x1[1, (plane - 1) * rows1 : (plane + 2) * rows1, :])

    mate.wait_recv()
    for plane in (2, 3):
        take_halo(plane, other, None)
    arrive(near)
    for plane, step in ((1, -1), (4, 1)):
        for side in range(2):
            take_halo(plane, side, valid(step))

    pooled = None
    for plane in (2, 3):
        pre = conv_one(plane)
        sig = jax.nn.sigmoid(pre)
        slopes[plane - 1] = sig * (1.0 + pre * (1.0 - sig))
        term = dot((pre * sig).astype(BF16), shrink[...])
        pooled = term if pooled is None else pooled + term
    pools[3] = pooled.astype(BF16)
    pool_copies = []
    for index, step in enumerate((1, -1, 2, -2, 3, -3)):
        one = copy(
            pools.at[3], pools.at[3 - step], send_p.at[index], recv_p.at[index], (at(step), core)
        )
        launch(one, step)
        pool_copies.append((one, step))

    arrive(far)
    for plane, step in ((0, -1), (5, 1)):
        for side in range(2):
            take_halo(plane, side, valid(step))
    for plane in (1, 4):
        slopes[plane - 1] = slope(conv_one(plane))

    def put_x2(plane, keep):
        field = pools[plane].astype(F32)
        if keep is not None:
            field = jnp.where(keep, field, 0.0)
        for tap, block in enumerate(plane_taps(field, across // 2)):
            for side in range(2):
                x2[side, pl.ds(plane * rows1 + tap * half, half), :] = block[
                    side * half : (side + 1) * half
                ]

    put_x2(3, None)
    arrive(cot_copies)
    arrive(pool_copies)
    for plane in (2, 4, 1, 5, 0, 6):
        put_x2(plane, valid(plane - 3))

    rows2 = 9 * outs
    own_grad = None
    for plane in range(5):
        pre = dot(w2f[0], x2[0, plane * rows1 : (plane + 3) * rows1, :])
        pre = pre + dot(w2f[1], x2[1, plane * rows1 : (plane + 3) * rows1, :])
        grad = cots[plane].reshape(outs, small).astype(F32) * slope(pre)
        if plane != 2:
            grad = jnp.where(valid(plane - 2), grad, 0.0)
        else:
            own_grad = grad.astype(BF16)
        grad = grad.astype(BF16)
        for tap, block in enumerate(plane_taps(grad, across // 2)):
            xg2[pl.ds((4 - plane) * rows2 + (8 - tap) * outs, outs), :] = block

    lanes = 512
    mine = place // stride
    is_owner = lax.rem(place, stride) == 0

    def when_owner(body):
        if stride == 1:
            body()
        else:
            pl.when(is_owner)(body)

    def chunk_out(total, part):
        rows = part.shape[1]
        for chunk in range(owners):
            r, l = chunk // 4, chunk % 4
            part[chunk] = total[r * rows : (r + 1) * rows, l * 128 : (l + 1) * 128].astype(BF16)

    def scatter_copy(part, land, send, recv, chunk, source, device):
        return copy(part.at[chunk], land.at[source], send.at[chunk], recv.at[source], device)

    def scatter(part, land, send, recv):
        def go(step, carry):
            chunk = lax.rem(mine + step, owners)

            @pl.when(chunk * stride != place)
            def _():
                scatter_copy(part, land, send, recv, chunk, place, (chunk * stride, core)).start()

            return carry

        lax.fori_loop(0, owners, go, 0)

        @when_owner
        def _():
            land[place] = part[mine]

    def gather(part, land, full, recv_r, send, recv):
        @when_owner
        def _():
            def arrived(step, carry):
                source = at(step)
                scatter_copy(part, land, send, recv_r, 0, source, (place, other)).wait_recv()
                return carry

            lax.fori_loop(1, n, arrived, 0)
            full[mine] = jnp.sum(land[...].astype(F32), axis=0).astype(BF16)

            def go(step, carry):
                copy(
                    full.at[mine], full.at[mine], send.at[at(step)], recv.at[mine], (at(step), core)
                ).start()
                return carry

            lax.fori_loop(1, n, go, 0)

    def finish(part, land, full, send_r, send, recv, out):
        def came(chunk, carry):
            @pl.when(chunk * stride != place)
            def _():
                copy(
                    full.at[chunk], full.at[chunk], send.at[0], recv.at[chunk], (place, other)
                ).wait_recv()
                scatter_copy(part, land, send_r, recv, chunk, 0, (place, other)).wait_send()

            return carry

        lax.fori_loop(0, owners, came, 0)

        @when_owner
        def _():
            def sent(step, carry):
                copy(
                    full.at[mine], full.at[mine], send.at[at(step)], recv.at[0], (place, other)
                ).wait_send()
                return carry

            lax.fori_loop(1, n, sent, 0)

        bands = [
            jnp.concatenate([full[4 * r + l].astype(F32) for l in range(4)], axis=1)
            for r in range(owners // 4)
        ]
        out[...] = jnp.concatenate(bands, axis=0).T[: out.shape[0]]

    total2 = dot_nt(own_grad, x2[core, 2 * rows1 : 2 * rows1 + lanes, :])
    chunk_out(total2, part2)
    scatter(part2, land2, send_r2, recv_r2)

    grads = []
    for plane in range(3):
        back = dot(w2b[...], xg2[(2 - plane) * rows2 : (5 - plane) * rows2, :]).astype(BF16)
        wide = dot(back, spread[...])
        for where in ((0,), (1, 2), (3,))[plane]:
            grad = wide * slopes[where]
            if plane != 1:
                grad = jnp.where(valid(plane - 1), grad, 0.0)
            grads.append(grad.astype(BF16))

    total1 = dot_nt(grads[1], x1[core, rows1 : rows1 + lanes, :])
    total1 = total1 + dot_nt(grads[2], x1[core, 2 * rows1 : 2 * rows1 + lanes, :])
    chunk_out(total1, part1)
    scatter(part1, land1, send_r1, recv_r1)
    gather(part2, land2, full2, recv_r2, send_a2, recv_a2)

    rows_g = 9 * mids
    for plane in range(4):
        for tap, block in enumerate(plane_taps(grads[plane], across)):
            xg1[pl.ds((3 - plane) * rows_g + (8 - tap) * mids, mids), :] = block
    for plane in range(2):
        field = dot(w1b[core], xg1[(1 - plane) * rows_g : (4 - plane) * rows_g, :])
        for row in range(rows):
            rel[plane, pl.ds(row, half, stride=rows), :] = field[
                :, row * across : (row + 1) * across
            ]
        out_feats[:, plane] = rel[plane].reshape(half, rows, across).astype(BF16)

    gather(part1, land1, full1, recv_r1, send_a1, recv_a1)
    mate.wait_send()
    leave(near + far + cot_copies + pool_copies)
    finish(part2, land2, full2, send_r2, send_a2, recv_a2, out_two)
    finish(part1, land1, full1, send_r1, send_a1, recv_a1, out_one)


def shards(feats, weight_one, weight_two, cotangent):
    n = lax.axis_size("depth")
    owners = 16
    half, planes, height, across = feats.shape
    cells = height * across
    mids = weight_one.shape[0]
    outs = weight_two.shape[0]
    small = cells // 4
    taps = weight_one.shape[2]
    w1 = jnp.transpose(weight_one, (2, 0, 1))
    w2 = jnp.transpose(weight_two, (2, 1, 0))
    vmem = pl.BlockSpec(memory_space=pltpu.VMEM)
    dma = pltpu.SemaphoreType.DMA
    out_feats, out_one, out_two = pl.pallas_call(
        functools.partial(kernel, n, owners, across),
        out_shape=(
            jax.ShapeDtypeStruct(feats.shape, BF16),
            jax.ShapeDtypeStruct((taps * half, mids), F32),
            jax.ShapeDtypeStruct((taps * half, outs), F32),
        ),
        in_specs=[vmem] * 4,
        out_specs=(vmem,) * 3,
        scratch_shapes=[
            pltpu.VMEM((planes, half, cells), BF16),
            pltpu.VMEM((planes, half * height, across), F32),
            pltpu.VMEM((outs // 2, small), BF16),
            pltpu.VMEM((outs // 2 * 8, across // 2), F32),
            pltpu.VMEM((2, mids, taps * half), BF16),
            pltpu.VMEM((2, half, taps * mids), BF16),
            pltpu.VMEM((2, outs, taps * half), BF16),
            pltpu.VMEM((mids, taps * outs), BF16),
            pltpu.VMEM((6, 2, half, cells), BF16),
            pltpu.VMEM((5, 2, outs // 2, small), BF16),
            pltpu.VMEM((7, mids, small), BF16),
            pltpu.VMEM((2, 6 * 9 * half, cells), BF16),
            pltpu.VMEM((2, 7 * 9 * half, small), BF16),
            pltpu.VMEM((4 * 9 * mids, cells), BF16),
            pltpu.VMEM((5 * 9 * outs, small), BF16),
            pltpu.VMEM((4, mids, cells), F32),
            pltpu.VMEM((cells, small), BF16),
            pltpu.VMEM((small, cells), BF16),
            pltpu.VMEM((owners, mids // 4, 128), BF16),
            pltpu.VMEM((n, mids // 4, 128), BF16),
            pltpu.VMEM((owners, mids // 4, 128), BF16),
            pltpu.VMEM((owners, outs // 4, 128), BF16),
            pltpu.VMEM((n, outs // 4, 128), BF16),
            pltpu.VMEM((owners, outs // 4, 128), BF16),
            dma((9,)), dma((9,)), dma((9,)), dma((9,)), dma((6,)), dma((6,)),
            dma((owners,)), dma((n,)), dma((n,)), dma((owners,)),
            dma((owners,)), dma((n,)), dma((n,)), dma((owners,)),
        ],
        compiler_params=pltpu.CompilerParams(
            collective_id=0, has_side_effects=True, vmem_limit_bytes=60 * 1024 * 1024
        ),
    )(feats, cotangent, w1, w2)

    def layout(total):
        return jnp.transpose(total.reshape(taps, half, total.shape[1]), (2, 1, 0))

    return out_feats, layout(out_one), layout(out_two)


def solution(mesh):
    return jax.shard_map(
        shards,
        mesh=mesh,
        in_specs=(P("chan", "depth", None, None), P(), P(), P("chan", "depth", None, None)),
        out_specs=(P("chan", "depth", None, None), P(None, "chan", None), P(None, "chan", None)),
        check_vma=False,
    )
```

```python
import functools

import jax
import jax.numpy as jnp
from jax import lax
from jax.experimental import pallas as pl
from jax.experimental.pallas import tpu as pltpu
from jax.sharding import PartitionSpec as P

MESH = pl.DeviceIdType.MESH
BF16 = jnp.bfloat16
F32 = jnp.float32


def dot(left, right):
    return jnp.dot(left, right, preferred_element_type=F32)


def dot_nt(left, right):
    return lax.dot_general(left, right, (((1,), (1,)), ((), ())), preferred_element_type=F32)


def slope(pre):
    sig = jax.nn.sigmoid(pre)
    return sig * (1.0 + pre * (1.0 - sig))


def plane_taps(field, across):
    chans, cells = field.shape
    wide = field.astype(F32)
    cell = lax.broadcasted_iota(jnp.int32, (chans, cells), 1)
    column = lax.rem(cell, across)
    moved = [
        jnp.where(column == 0, 0.0, pltpu.roll(wide, 1, 1)),
        wide,
        jnp.where(column == across - 1, 0.0, pltpu.roll(wide, cells - 1, 1)),
    ]
    if across % 128 == 0:
        moved = [m.astype(BF16) for m in moved]
        edge = jnp.zeros((chans, across), BF16)
        above = [jnp.concatenate([edge, m[:, :-across]], axis=1) for m in moved]
        below = [jnp.concatenate([m[:, across:], edge], axis=1) for m in moved]
        return above + moved + below
    above = [jnp.where(cell < across, 0.0, pltpu.roll(m, across, 1)) for m in moved]
    below = [
        jnp.where(cell >= cells - across, 0.0, pltpu.roll(m, cells - across, 1)) for m in moved
    ]
    return [m.astype(BF16) for m in above + moved + below]


def kernel(
    n, owners, across,
    feats_in, cot_in, w1, w2,
    out_feats, out_one, out_two,
    feats, rel, cot, crel, w1f, w1b, w2f, w2b, halo, cots, pools, x1, x2, xg1, xg2, slopes, edges, beyond, shrink, spread,
    part1, land1, full1, part2, land2, full2,
    send_f, recv_f, send_c, recv_c, send_p, recv_p, send_e, recv_e,
    send_r1, recv_r1, send_a1, recv_a1, send_r2, recv_r2, send_a2, recv_a2,
):
    place = lax.axis_index("depth")
    core = lax.axis_index("chan")
    other = 1 - core
    half = feats.shape[1]
    cells = feats.shape[2]
    small = cot.shape[1]
    rows1 = 9 * half
    stride = n // owners

    def at(step):
        return lax.rem(place + step + n, n)

    barrier = pltpu.get_barrier_semaphore()

    def greet(device):
        pl.semaphore_signal(barrier, inc=1, device_id=device, device_id_type=MESH)

    greet((place, other))
    for step in (1, -1, 2, -2):
        greet((at(step), other))

    def greet_row(step, carry):
        greet((at(step), core))
        return carry

    lax.fori_loop(1, n, greet_row, 0)

    def valid(step):
        return jnp.logical_and(place + step >= 0, place + step < n)

    def put_x1(plane, side, field):
        for tap, block in enumerate(plane_taps(field, across)):
            x1[side, pl.ds(plane * rows1 + tap * half, half), :] = block

    big_row = lax.broadcasted_iota(jnp.int32, (cells, small), 0)
    small_col = lax.broadcasted_iota(jnp.int32, (cells, small), 1)
    target = (big_row // (2 * across)) * (across // 2) + lax.rem(big_row, across) // 2
    shrink[...] = jnp.where(target == small_col, 0.125, 0.0).astype(BF16)
    big_col = lax.broadcasted_iota(jnp.int32, (small, cells), 1)
    small_row = lax.broadcasted_iota(jnp.int32, (small, cells), 0)
    target = (big_col // (2 * across)) * (across // 2) + lax.rem(big_col, across) // 2
    spread[...] = jnp.where(target == small_row, 0.125, 0.0).astype(BF16)

    rows = cells // across
    x1[:, 4 * rows1 :, :] = jnp.zeros((2, x1.shape[1] - 4 * rows1, cells), BF16)
    for plane in range(2):
        rel[plane] = feats_in[:, plane].astype(F32).reshape(half * rows, across)
        for row in range(rows):
            feats[plane, :, row * across : (row + 1) * across] = rel[
                plane, pl.ds(row, half, stride=rows), :
            ].astype(BF16)
        put_x1(1 + plane, core, feats[plane])
    short = small // (across // 2)
    for chan in range(cot.shape[0]):
        crel[chan * 8 : chan * 8 + short, :] = cot_in[chan, 0].astype(F32)
    lines = [crel[pl.ds(row, cot.shape[0], stride=8), :] for row in range(short)]
    cot[...] = jnp.concatenate(lines, axis=1).astype(BF16)
    cots[2, core] = cot[...]

    taps, mids, _ = w1.shape
    outs = w2.shape[2]
    for side in range(2):
        lo, hi = side * half, (side + 1) * half
        for tap in range(taps):
            w1f[side, :, tap * half : (tap + 1) * half] = w1[tap][:, lo:hi]
        w2f[side] = w2[:, lo:hi, :].reshape(taps * half, outs).T
    w1b[...] = w1[...].reshape(taps * mids, mids).T.reshape(2, half, taps * mids)
    for tap in range(taps):
        w2b[:, tap * outs : (tap + 1) * outs] = w2[tap]

    pl.semaphore_wait(barrier, n + 4)

    def copy(src, dst, send, recv, device):
        return pltpu.make_async_remote_copy(
            src_ref=src, dst_ref=dst, send_sem=send, recv_sem=recv,
            device_id=device, device_id_type=MESH,
        )

    def launch(one, step):
        pl.when(valid(step))(lambda: one.start())

    def arrive(pairs):
        for one, step in pairs:
            pl.when(valid(-step))(lambda one=one: one.wait_recv())

    def leave(pairs):
        for one, step in pairs:
            pl.when(valid(step))(lambda one=one: one.wait_send())

    near = []
    mate = copy(feats, halo.at[pl.ds(1, 2), core], send_f.at[0], recv_f.at[0], (place, other))
    mate.start()
    index = 1
    for step, plane, to in ((1, 1, 0), (-1, 0, 3)):
        for who in (core, other):
            one = copy(
                feats.at[plane], halo.at[to, core], send_f.at[index], recv_f.at[index],
                (at(step), who),
            )
            launch(one, step)
            near.append((one, step))
            index += 1
    cot_copies = []
    index = 0
    targets = [(0, other)] + [(s, w) for s in (1, -1, 2, -2) for w in (core, other)]
    for step, who in targets:
        one = copy(
            cot, cots.at[2 - step, core], send_c.at[index], recv_c.at[index], (at(step), who)
        )
        launch(one, step)
        cot_copies.append((one, step))
        index += 1

    def take_halo(plane, side, keep):
        field = halo[plane, side]
        if keep is not None:
            field = jnp.where(keep, field.astype(F32), 0.0)
        put_x1(plane, side, field)

    def conv_one(plane):
        total = dot(w1f[0], x1[0, (plane - 1) * rows1 : (plane + 2) * rows1, :])
        return total + dot(w1f[1], x1[1, (plane - 1) * rows1 : (plane + 2) * rows1, :])

    mate.wait_recv()
    for plane in (1, 2):
        take_halo(plane, other, None)
    arrive(near)
    for plane, step in ((0, -1), (3, 1)):
        for side in range(2):
            take_halo(plane, side, valid(step))

    pooled = None
    for plane in range(2):
        pre = conv_one(plane + 1)
        sig = jax.nn.sigmoid(pre)
        bend = sig * (1.0 + pre * (1.0 - sig))
        slopes[plane] = bend
        edges[plane] = bend.astype(BF16)
        term = dot((pre * sig).astype(BF16), shrink[...])
        pooled = term if pooled is None else pooled + term
    pools[3] = pooled.astype(BF16)
    pool_copies = []
    for index, step in enumerate((1, -1, 2, -2, 3, -3)):
        one = copy(
            pools.at[3], pools.at[3 - step], send_p.at[index], recv_p.at[index], (at(step), core)
        )
        launch(one, step)
        pool_copies.append((one, step))

    edge_copies = []
    for index, step in enumerate((1, -1)):
        one = copy(
            edges.at[1 - index], beyond.at[index], send_e.at[index], recv_e.at[index],
            (at(step), core),
        )
        launch(one, step)
        edge_copies.append((one, step))

    def put_x2(plane, keep):
        field = pools[plane].astype(F32)
        if keep is not None:
            field = jnp.where(keep, field, 0.0)
        for tap, block in enumerate(plane_taps(field, across // 2)):
            for side in range(2):
                x2[side, pl.ds(plane * rows1 + tap * half, half), :] = block[
                    side * half : (side + 1) * half
                ]

    rows2 = 9 * outs

    def level_two(plane):
        pre = dot(w2f[0], x2[0, plane * rows1 : (plane + 3) * rows1, :])
        pre = pre + dot(w2f[1], x2[1, plane * rows1 : (plane + 3) * rows1, :])
        grad = cots[plane].reshape(outs, small).astype(F32) * slope(pre)
        if plane != 2:
            grad = jnp.where(valid(plane - 2), grad, 0.0)
        return grad.astype(BF16)

    def put_xg2(plane, grad):
        for tap, block in enumerate(plane_taps(grad, across // 2)):
            xg2[pl.ds((4 - plane) * rows2 + (8 - tap) * outs, outs), :] = block

    def back(plane):
        total = dot(w2b[...], xg2[(2 - plane) * rows2 : (5 - plane) * rows2, :])
        return dot(total.astype(BF16), spread[...])

    lanes = 512
    mine = place // stride
    is_owner = lax.rem(place, stride) == 0

    def when_owner(body):
        if stride == 1:
            body()
        else:
            pl.when(is_owner)(body)

    def chunk_out(total, part):
        rows = part.shape[1]
        for chunk in range(owners):
            r, l = chunk // 4, chunk % 4
            part[chunk] = total[r * rows : (r + 1) * rows, l * 128 : (l + 1) * 128].astype(BF16)

    def scatter_copy(part, land, send, recv, chunk, source, device):
        return copy(part.at[chunk], land.at[source], send.at[chunk], recv.at[source], device)

    def scatter(part, land, send, recv):
        def go(step, carry):
            chunk = lax.rem(mine + step, owners)

            @pl.when(chunk * stride != place)
            def _():
                scatter_copy(part, land, send, recv, chunk, place, (chunk * stride, core)).start()

            return carry

        lax.fori_loop(0, owners, go, 0)

        @when_owner
        def _():
            land[place] = part[mine]

    def gather(part, land, full, recv_r, send, recv):
        @when_owner
        def _():
            def arrived(step, carry):
                source = at(step)
                scatter_copy(part, land, send, recv_r, 0, source, (place, other)).wait_recv()
                return carry

            lax.fori_loop(1, n, arrived, 0)
            full[mine] = jnp.sum(land[...].astype(F32), axis=0).astype(BF16)

            def go(step, carry):
                copy(
                    full.at[mine], full.at[mine], send.at[at(step)], recv.at[mine], (at(step), core)
                ).start()
                return carry

            lax.fori_loop(1, n, go, 0)

    def finish(part, land, full, send_r, send, recv, out):
        def came(chunk, carry):
            @pl.when(chunk * stride != place)
            def _():
                copy(
                    full.at[chunk], full.at[chunk], send.at[0], recv.at[chunk], (place, other)
                ).wait_recv()
                scatter_copy(part, land, send_r, recv, chunk, 0, (place, other)).wait_send()

            return carry

        lax.fori_loop(0, owners, came, 0)

        @when_owner
        def _():
            def sent(step, carry):
                copy(
                    full.at[mine], full.at[mine], send.at[at(step)], recv.at[0], (place, other)
                ).wait_send()
                return carry

            lax.fori_loop(1, n, sent, 0)

        bands = [
            jnp.concatenate([full[4 * r + l].astype(F32) for l in range(4)], axis=1)
            for r in range(owners // 4)
        ]
        out[...] = jnp.concatenate(bands, axis=0).T[: out.shape[0]]

    put_x2(3, None)
    arrive(cot_copies[:1])
    arrive(pool_copies[:2])
    for plane in (2, 4):
        put_x2(plane, valid(plane - 3))
    grad = level_two(2)
    total2 = dot_nt(grad, x2[core, 2 * rows1 : 2 * rows1 + lanes, :])
    chunk_out(total2, part2)
    scatter(part2, land2, send_r2, recv_r2)
    put_xg2(2, grad)

    arrive(cot_copies[1:5])
    arrive(pool_copies[2:4])
    for plane in (1, 5):
        put_x2(plane, valid(plane - 3))
    for plane in (1, 3):
        put_xg2(plane, level_two(plane))

    wide = back(1)
    inner = [(wide * slopes[plane]).astype(BF16) for plane in range(2)]
    total1 = dot_nt(inner[0], x1[core, :lanes, :])
    total1 = total1 + dot_nt(inner[1], x1[core, rows1 : rows1 + lanes, :])
    chunk_out(total1, part1)
    scatter(part1, land1, send_r1, recv_r1)

    arrive(cot_copies[5:])
    arrive(pool_copies[4:])
    for plane in (0, 6):
        put_x2(plane, valid(plane - 3))
    for plane in (0, 4):
        put_xg2(plane, level_two(plane))
    arrive(edge_copies)
    outer = []
    for index, step in enumerate((-1, 1)):
        grad = back(1 + step) * beyond[index].astype(F32)
        outer.append(jnp.where(valid(step), grad, 0.0).astype(BF16))
    grads = [outer[0], inner[0], inner[1], outer[1]]
    gather(part2, land2, full2, recv_r2, send_a2, recv_a2)

    rows_g = 9 * mids
    for plane in range(4):
        for tap, block in enumerate(plane_taps(grads[plane], across)):
            xg1[pl.ds((3 - plane) * rows_g + (8 - tap) * mids, mids), :] = block
    for plane in range(2):
        field = dot(w1b[core], xg1[(1 - plane) * rows_g : (4 - plane) * rows_g, :])
        for row in range(rows):
            rel[plane, pl.ds(row, half, stride=rows), :] = field[
                :, row * across : (row + 1) * across
            ]
        out_feats[:, plane] = rel[plane].reshape(half, rows, across).astype(BF16)

    gather(part1, land1, full1, recv_r1, send_a1, recv_a1)
    mate.wait_send()
    leave(near + cot_copies + pool_copies + edge_copies)
    finish(part2, land2, full2, send_r2, send_a2, recv_a2, out_two)
    finish(part1, land1, full1, send_r1, send_a1, recv_a1, out_one)


def shards(feats, weight_one, weight_two, cotangent):
    n = lax.axis_size("depth")
    owners = 16
    half, planes, height, across = feats.shape
    cells = height * across
    mids = weight_one.shape[0]
    outs = weight_two.shape[0]
    small = cells // 4
    taps = weight_one.shape[2]
    w1 = jnp.transpose(weight_one, (2, 0, 1))
    w2 = jnp.transpose(weight_two, (2, 1, 0))
    vmem = pl.BlockSpec(memory_space=pltpu.VMEM)
    dma = pltpu.SemaphoreType.DMA
    out_feats, out_one, out_two = pl.pallas_call(
        functools.partial(kernel, n, owners, across),
        out_shape=(
            jax.ShapeDtypeStruct(feats.shape, BF16),
            jax.ShapeDtypeStruct((taps * half, mids), F32),
            jax.ShapeDtypeStruct((taps * half, outs), F32),
        ),
        in_specs=[vmem] * 4,
        out_specs=(vmem,) * 3,
        scratch_shapes=[
            pltpu.VMEM((planes, half, cells), BF16),
            pltpu.VMEM((planes, half * height, across), F32),
            pltpu.VMEM((outs // 2, small), BF16),
            pltpu.VMEM((outs // 2 * 8, across // 2), F32),
            pltpu.VMEM((2, mids, taps * half), BF16),
            pltpu.VMEM((2, half, taps * mids), BF16),
            pltpu.VMEM((2, outs, taps * half), BF16),
            pltpu.VMEM((mids, taps * outs), BF16),
            pltpu.VMEM((4, 2, half, cells), BF16),
            pltpu.VMEM((5, 2, outs // 2, small), BF16),
            pltpu.VMEM((7, mids, small), BF16),
            pltpu.VMEM((2, 5 * 9 * half, cells), BF16),
            pltpu.VMEM((2, 7 * 9 * half, small), BF16),
            pltpu.VMEM((4 * 9 * mids, cells), BF16),
            pltpu.VMEM((5 * 9 * outs, small), BF16),
            pltpu.VMEM((2, mids, cells), F32),
            pltpu.VMEM((2, mids, cells), BF16),
            pltpu.VMEM((2, mids, cells), BF16),
            pltpu.VMEM((cells, small), BF16),
            pltpu.VMEM((small, cells), BF16),
            pltpu.VMEM((owners, mids // 4, 128), BF16),
            pltpu.VMEM((n, mids // 4, 128), BF16),
            pltpu.VMEM((owners, mids // 4, 128), BF16),
            pltpu.VMEM((owners, outs // 4, 128), BF16),
            pltpu.VMEM((n, outs // 4, 128), BF16),
            pltpu.VMEM((owners, outs // 4, 128), BF16),
            dma((5,)), dma((5,)), dma((9,)), dma((9,)), dma((6,)), dma((6,)), dma((2,)), dma((2,)),
            dma((owners,)), dma((n,)), dma((n,)), dma((owners,)),
            dma((owners,)), dma((n,)), dma((n,)), dma((owners,)),
        ],
        compiler_params=pltpu.CompilerParams(
            collective_id=0, has_side_effects=True, vmem_limit_bytes=60 * 1024 * 1024
        ),
    )(feats, cotangent, w1, w2)

    def layout(total):
        return jnp.transpose(total.reshape(taps, half, total.shape[1]), (2, 1, 0))

    return out_feats, layout(out_one), layout(out_two)


def solution(mesh):
    return jax.shard_map(
        shards,
        mesh=mesh,
        in_specs=(P("chan", "depth", None, None), P(), P(), P("chan", "depth", None, None)),
        out_specs=(P("chan", "depth", None, None), P(None, "chan", None), P(None, "chan", None)),
        check_vma=False,
    )
```

```python
import functools

import jax
import jax.numpy as jnp
from jax import lax
from jax.experimental import pallas as pl
from jax.experimental.pallas import tpu as pltpu
from jax.sharding import PartitionSpec as P

MESH = pl.DeviceIdType.MESH
BF16 = jnp.bfloat16
F32 = jnp.float32


def dot(left, right):
    return jnp.dot(left, right, preferred_element_type=F32)


def dot_nt(left, right):
    return lax.dot_general(left, right, (((1,), (1,)), ((), ())), preferred_element_type=F32)


def slope(pre):
    sig = jax.nn.sigmoid(pre)
    return sig * (1.0 + pre * (1.0 - sig))


def plane_taps(field, across):
    chans, cells = field.shape
    wide = field.astype(F32)
    cell = lax.broadcasted_iota(jnp.int32, (chans, cells), 1)
    column = lax.rem(cell, across)
    moved = [
        jnp.where(column == 0, 0.0, pltpu.roll(wide, 1, 1)),
        wide,
        jnp.where(column == across - 1, 0.0, pltpu.roll(wide, cells - 1, 1)),
    ]
    if across % 128 == 0:
        moved = [m.astype(BF16) for m in moved]
        edge = jnp.zeros((chans, across), BF16)
        above = [jnp.concatenate([edge, m[:, :-across]], axis=1) for m in moved]
        below = [jnp.concatenate([m[:, across:], edge], axis=1) for m in moved]
        return above + moved + below
    above = [jnp.where(cell < across, 0.0, pltpu.roll(m, across, 1)) for m in moved]
    below = [
        jnp.where(cell >= cells - across, 0.0, pltpu.roll(m, cells - across, 1)) for m in moved
    ]
    return [m.astype(BF16) for m in above + moved + below]


def kernel(
    n, owners, across,
    feats_hbm, cot_hbm, w1_hbm, w2_hbm,
    out_feats, out_one, out_two,
    feats_in, cot_in, w1, w2, feats, rel, cot, crel, w1f, w1b, w2f, w2b, halo, cots, pools, x1, x2, xg1, xg2, slopes, edges, beyond, shrink, spread,
    part1, land1, full1, part2, land2, full2,
    send_f, recv_f, send_c, recv_c, load, send_p, recv_p, send_e, recv_e,
    send_r1, recv_r1, send_a1, recv_a1, send_r2, recv_r2, send_a2, recv_a2,
):
    place = lax.axis_index("depth")
    core = lax.axis_index("chan")
    other = 1 - core
    half = feats.shape[1]
    cells = feats.shape[2]
    small = cot.shape[1]
    rows1 = 9 * half
    stride = n // owners

    def at(step):
        return lax.rem(place + step + n, n)

    barrier = pltpu.get_barrier_semaphore()

    def greet(device):
        pl.semaphore_signal(barrier, inc=1, device_id=device, device_id_type=MESH)

    greet((place, other))
    for step in (1, -1, 2, -2):
        greet((at(step), other))

    def greet_row(step, carry):
        greet((at(step), core))
        return carry

    lax.fori_loop(1, n, greet_row, 0)

    loads = [
        pltpu.make_async_copy(source, target, load.at[index])
        for index, (source, target) in enumerate(
            ((feats_hbm, feats_in), (cot_hbm, cot_in), (w1_hbm, w1), (w2_hbm, w2))
        )
    ]
    for one in loads:
        one.start()

    def valid(step):
        return jnp.logical_and(place + step >= 0, place + step < n)

    def put_x1(plane, side, field):
        for tap, block in enumerate(plane_taps(field, across)):
            x1[side, pl.ds(plane * rows1 + tap * half, half), :] = block

    rows = cells // across
    loads[0].wait()
    for plane in range(2):
        rel[plane] = feats_in[:, plane].astype(F32).reshape(half * rows, across)
        for row in range(rows):
            feats[plane, :, row * across : (row + 1) * across] = rel[
                plane, pl.ds(row, half, stride=rows), :
            ].astype(BF16)
    loads[1].wait()
    short = small // (across // 2)
    for chan in range(cot.shape[0]):
        crel[chan * 8 : chan * 8 + short, :] = cot_in[chan, 0].astype(F32)
    lines = [crel[pl.ds(row, cot.shape[0], stride=8), :] for row in range(short)]
    cot[...] = jnp.concatenate(lines, axis=1).astype(BF16)
    pl.semaphore_wait(barrier, n + 4)

    def copy(src, dst, send, recv, device):
        return pltpu.make_async_remote_copy(
            src_ref=src, dst_ref=dst, send_sem=send, recv_sem=recv,
            device_id=device, device_id_type=MESH,
        )

    def launch(one, step):
        pl.when(valid(step))(lambda: one.start())

    def arrive(pairs):
        for one, step in pairs:
            pl.when(valid(-step))(lambda one=one: one.wait_recv())

    def leave(pairs):
        for one, step in pairs:
            pl.when(valid(step))(lambda one=one: one.wait_send())

    near = []
    mate = copy(feats, halo.at[pl.ds(1, 2), core], send_f.at[0], recv_f.at[0], (place, other))
    mate.start()
    index = 1
    for step, plane, to in ((1, 1, 0), (-1, 0, 3)):
        for who in (core, other):
            one = copy(
                feats.at[plane], halo.at[to, core], send_f.at[index], recv_f.at[index],
                (at(step), who),
            )
            launch(one, step)
            near.append((one, step))
            index += 1
    cot_copies = []
    index = 0
    targets = [(0, other)] + [(s, w) for s in (1, -1, 2, -2) for w in (core, other)]
    for step, who in targets:
        one = copy(
            cot, cots.at[2 - step, core], send_c.at[index], recv_c.at[index], (at(step), who)
        )
        launch(one, step)
        cot_copies.append((one, step))
        index += 1

    def take_halo(plane, side, keep):
        field = halo[plane, side]
        if keep is not None:
            field = jnp.where(keep, field.astype(F32), 0.0)
        put_x1(plane, side, field)

    def conv_one(plane):
        total = dot(w1f[0], x1[0, (plane - 1) * rows1 : (plane + 2) * rows1, :])
        return total + dot(w1f[1], x1[1, (plane - 1) * rows1 : (plane + 2) * rows1, :])

    cots[2, core] = cot[...]

    for plane in range(2):
        put_x1(1 + plane, core, feats[plane])
    x1[:, 4 * rows1 :, :] = jnp.zeros((2, x1.shape[1] - 4 * rows1, cells), BF16)
    loads[2].wait()
    loads[3].wait()
    taps, mids, _ = w1.shape
    outs = w2.shape[2]
    for side in range(2):
        lo, hi = side * half, (side + 1) * half
        for tap in range(taps):
            w1f[side, :, tap * half : (tap + 1) * half] = w1[tap][:, lo:hi]
        w2f[side] = w2[:, lo:hi, :].reshape(taps * half, outs).T
    w1b[...] = w1[...].reshape(taps * mids, mids).T.reshape(2, half, taps * mids)
    for tap in range(taps):
        w2b[:, tap * outs : (tap + 1) * outs] = w2[tap]
    big_row = lax.broadcasted_iota(jnp.int32, (cells, small), 0)
    small_col = lax.broadcasted_iota(jnp.int32, (cells, small), 1)
    target = (big_row // (2 * across)) * (across // 2) + lax.rem(big_row, across) // 2
    shrink[...] = jnp.where(target == small_col, 0.125, 0.0).astype(BF16)
    big_col = lax.broadcasted_iota(jnp.int32, (small, cells), 1)
    small_row = lax.broadcasted_iota(jnp.int32, (small, cells), 0)
    target = (big_col // (2 * across)) * (across // 2) + lax.rem(big_col, across) // 2
    spread[...] = jnp.where(target == small_row, 0.125, 0.0).astype(BF16)

    mate.wait_recv()
    for plane in (1, 2):
        take_halo(plane, other, None)
    arrive(near)
    for plane, step in ((0, -1), (3, 1)):
        for side in range(2):
            take_halo(plane, side, valid(step))

    pooled = None
    for plane in range(2):
        pre = conv_one(plane + 1)
        sig = jax.nn.sigmoid(pre)
        bend = sig * (1.0 + pre * (1.0 - sig))
        slopes[plane] = bend
        edges[plane] = bend.astype(BF16)
        term = dot((pre * sig).astype(BF16), shrink[...])
        pooled = term if pooled is None else pooled + term
    pools[3] = pooled.astype(BF16)
    pool_copies = []
    for index, step in enumerate((1, -1, 2, -2, 3, -3)):
        one = copy(
            pools.at[3], pools.at[3 - step], send_p.at[index], recv_p.at[index], (at(step), core)
        )
        launch(one, step)
        pool_copies.append((one, step))

    edge_copies = []
    for index, step in enumerate((1, -1)):
        one = copy(
            edges.at[1 - index], beyond.at[index], send_e.at[index], recv_e.at[index],
            (at(step), core),
        )
        launch(one, step)
        edge_copies.append((one, step))

    def put_x2(plane, keep):
        field = pools[plane].astype(F32)
        if keep is not None:
            field = jnp.where(keep, field, 0.0)
        for tap, block in enumerate(plane_taps(field, across // 2)):
            for side in range(2):
                x2[side, pl.ds(plane * rows1 + tap * half, half), :] = block[
                    side * half : (side + 1) * half
                ]

    rows2 = 9 * outs

    def level_two(plane):
        pre = dot(w2f[0], x2[0, plane * rows1 : (plane + 3) * rows1, :])
        pre = pre + dot(w2f[1], x2[1, plane * rows1 : (plane + 3) * rows1, :])
        grad = cots[plane].reshape(outs, small).astype(F32) * slope(pre)
        if plane != 2:
            grad = jnp.where(valid(plane - 2), grad, 0.0)
        return grad.astype(BF16)

    def put_xg2(plane, grad):
        for tap, block in enumerate(plane_taps(grad, across // 2)):
            xg2[pl.ds((4 - plane) * rows2 + (8 - tap) * outs, outs), :] = block

    def back(plane):
        total = dot(w2b[...], xg2[(2 - plane) * rows2 : (5 - plane) * rows2, :])
        return dot(total.astype(BF16), spread[...])

    lanes = 512
    mine = place // stride
    is_owner = lax.rem(place, stride) == 0

    def when_owner(body):
        if stride == 1:
            body()
        else:
            pl.when(is_owner)(body)

    def chunk_out(total, part):
        rows = part.shape[1]
        for chunk in range(owners):
            r, l = chunk // 4, chunk % 4
            part[chunk] = total[r * rows : (r + 1) * rows, l * 128 : (l + 1) * 128].astype(BF16)

    def scatter_copy(part, land, send, recv, chunk, source, device):
        return copy(part.at[chunk], land.at[source], send.at[chunk], recv.at[source], device)

    def scatter(part, land, send, recv):
        def go(step, carry):
            chunk = lax.rem(mine + step, owners)

            @pl.when(chunk * stride != place)
            def _():
                scatter_copy(part, land, send, recv, chunk, place, (chunk * stride, core)).start()

            return carry

        lax.fori_loop(0, owners, go, 0)

        @when_owner
        def _():
            land[place] = part[mine]

    def gather(part, land, full, recv_r, send, recv):
        @when_owner
        def _():
            def arrived(step, carry):
                source = at(step)
                scatter_copy(part, land, send, recv_r, 0, source, (place, other)).wait_recv()
                return carry

            lax.fori_loop(1, n, arrived, 0)
            full[mine] = jnp.sum(land[...].astype(F32), axis=0).astype(BF16)

            def go(step, carry):
                copy(
                    full.at[mine], full.at[mine], send.at[at(step)], recv.at[mine], (at(step), core)
                ).start()
                return carry

            lax.fori_loop(1, n, go, 0)

    def finish(part, land, full, send_r, send, recv, out):
        def came(chunk, carry):
            @pl.when(chunk * stride != place)
            def _():
                copy(
                    full.at[chunk], full.at[chunk], send.at[0], recv.at[chunk], (place, other)
                ).wait_recv()
                scatter_copy(part, land, send_r, recv, chunk, 0, (place, other)).wait_send()

            return carry

        lax.fori_loop(0, owners, came, 0)

        @when_owner
        def _():
            def sent(step, carry):
                copy(
                    full.at[mine], full.at[mine], send.at[at(step)], recv.at[0], (place, other)
                ).wait_send()
                return carry

            lax.fori_loop(1, n, sent, 0)

        bands = [
            jnp.concatenate([full[4 * r + l].astype(F32) for l in range(4)], axis=1)
            for r in range(owners // 4)
        ]
        out[...] = jnp.concatenate(bands, axis=0).T[: out.shape[0]]

    put_x2(3, None)
    arrive(cot_copies[:1])
    arrive(pool_copies[:2])
    for plane in (2, 4):
        put_x2(plane, valid(plane - 3))
    grad = level_two(2)
    total2 = dot_nt(grad, x2[core, 2 * rows1 : 2 * rows1 + lanes, :])
    chunk_out(total2, part2)
    scatter(part2, land2, send_r2, recv_r2)
    put_xg2(2, grad)

    arrive(cot_copies[1:5])
    arrive(pool_copies[2:4])
    for plane in (1, 5):
        put_x2(plane, valid(plane - 3))
    for plane in (1, 3):
        put_xg2(plane, level_two(plane))

    wide = back(1)
    inner = [(wide * slopes[plane]).astype(BF16) for plane in range(2)]
    total1 = dot_nt(inner[0], x1[core, :lanes, :])
    total1 = total1 + dot_nt(inner[1], x1[core, rows1 : rows1 + lanes, :])
    chunk_out(total1, part1)
    scatter(part1, land1, send_r1, recv_r1)

    arrive(cot_copies[5:])
    arrive(pool_copies[4:])
    for plane in (0, 6):
        put_x2(plane, valid(plane - 3))
    for plane in (0, 4):
        put_xg2(plane, level_two(plane))
    arrive(edge_copies)
    outer = []
    for index, step in enumerate((-1, 1)):
        grad = back(1 + step) * beyond[index].astype(F32)
        outer.append(jnp.where(valid(step), grad, 0.0).astype(BF16))
    grads = [outer[0], inner[0], inner[1], outer[1]]
    gather(part2, land2, full2, recv_r2, send_a2, recv_a2)

    rows_g = 9 * mids
    for plane in range(4):
        for tap, block in enumerate(plane_taps(grads[plane], across)):
            xg1[pl.ds((3 - plane) * rows_g + (8 - tap) * mids, mids), :] = block
    for plane in range(2):
        field = dot(w1b[core], xg1[(1 - plane) * rows_g : (4 - plane) * rows_g, :])
        for row in range(rows):
            rel[plane, pl.ds(row, half, stride=rows), :] = field[
                :, row * across : (row + 1) * across
            ]
        out_feats[:, plane] = rel[plane].reshape(half, rows, across).astype(BF16)

    gather(part1, land1, full1, recv_r1, send_a1, recv_a1)
    mate.wait_send()
    leave(near + cot_copies + pool_copies + edge_copies)
    finish(part2, land2, full2, send_r2, send_a2, recv_a2, out_two)
    finish(part1, land1, full1, send_r1, send_a1, recv_a1, out_one)


def shards(feats, weight_one, weight_two, cotangent):
    n = lax.axis_size("depth")
    owners = 16
    half, planes, height, across = feats.shape
    cells = height * across
    mids = weight_one.shape[0]
    outs = weight_two.shape[0]
    small = cells // 4
    taps = weight_one.shape[2]
    w1 = jnp.transpose(weight_one, (2, 0, 1))
    w2 = jnp.transpose(weight_two, (2, 1, 0))
    vmem = pl.BlockSpec(memory_space=pltpu.VMEM)
    dma = pltpu.SemaphoreType.DMA
    out_feats, out_one, out_two = pl.pallas_call(
        functools.partial(kernel, n, owners, across),
        out_shape=(
            jax.ShapeDtypeStruct(feats.shape, BF16),
            jax.ShapeDtypeStruct((taps * half, mids), F32),
            jax.ShapeDtypeStruct((taps * half, outs), F32),
        ),
        in_specs=[pl.BlockSpec(memory_space=pl.ANY)] * 4,
        out_specs=(vmem,) * 3,
        scratch_shapes=[
            pltpu.VMEM(feats.shape, BF16),
            pltpu.VMEM(cotangent.shape, BF16),
            pltpu.VMEM(w1.shape, BF16),
            pltpu.VMEM(w2.shape, BF16),
            pltpu.VMEM((planes, half, cells), BF16),
            pltpu.VMEM((planes, half * height, across), F32),
            pltpu.VMEM((outs // 2, small), BF16),
            pltpu.VMEM((outs // 2 * 8, across // 2), F32),
            pltpu.VMEM((2, mids, taps * half), BF16),
            pltpu.VMEM((2, half, taps * mids), BF16),
            pltpu.VMEM((2, outs, taps * half), BF16),
            pltpu.VMEM((mids, taps * outs), BF16),
            pltpu.VMEM((4, 2, half, cells), BF16),
            pltpu.VMEM((5, 2, outs // 2, small), BF16),
            pltpu.VMEM((7, mids, small), BF16),
            pltpu.VMEM((2, 5 * 9 * half, cells), BF16),
            pltpu.VMEM((2, 7 * 9 * half, small), BF16),
            pltpu.VMEM((4 * 9 * mids, cells), BF16),
            pltpu.VMEM((5 * 9 * outs, small), BF16),
            pltpu.VMEM((2, mids, cells), F32),
            pltpu.VMEM((2, mids, cells), BF16),
            pltpu.VMEM((2, mids, cells), BF16),
            pltpu.VMEM((cells, small), BF16),
            pltpu.VMEM((small, cells), BF16),
            pltpu.VMEM((owners, mids // 4, 128), BF16),
            pltpu.VMEM((n, mids // 4, 128), BF16),
            pltpu.VMEM((owners, mids // 4, 128), BF16),
            pltpu.VMEM((owners, outs // 4, 128), BF16),
            pltpu.VMEM((n, outs // 4, 128), BF16),
            pltpu.VMEM((owners, outs // 4, 128), BF16),
            dma((5,)), dma((5,)), dma((9,)), dma((9,)), dma((4,)), dma((6,)), dma((6,)), dma((2,)), dma((2,)),
            dma((owners,)), dma((n,)), dma((n,)), dma((owners,)),
            dma((owners,)), dma((n,)), dma((n,)), dma((owners,)),
        ],
        compiler_params=pltpu.CompilerParams(
            collective_id=0, has_side_effects=True, vmem_limit_bytes=60 * 1024 * 1024
        ),
    )(feats, cotangent, w1, w2)

    def layout(total):
        return jnp.transpose(total.reshape(taps, half, total.shape[1]), (2, 1, 0))

    return out_feats, layout(out_one), layout(out_two)


def solution(mesh):
    return jax.shard_map(
        shards,
        mesh=mesh,
        in_specs=(P("chan", "depth", None, None), P(), P(), P("chan", "depth", None, None)),
        out_specs=(P("chan", "depth", None, None), P(None, "chan", None), P(None, "chan", None)),
        check_vma=False,
    )
```

```python
import functools

import jax
import jax.numpy as jnp
from jax import lax
from jax.experimental import pallas as pl
from jax.experimental.pallas import tpu as pltpu
from jax.sharding import PartitionSpec as P

MESH = pl.DeviceIdType.MESH
BF16 = jnp.bfloat16
F32 = jnp.float32


def dot(left, right):
    return jnp.dot(left, right, preferred_element_type=F32)


def dot_nt(left, right):
    return lax.dot_general(left, right, (((1,), (1,)), ((), ())), preferred_element_type=F32)


def slope(pre):
    sig = jax.nn.sigmoid(pre)
    return sig * (1.0 + pre * (1.0 - sig))


def plane_taps(field, across):
    chans, cells = field.shape
    wide = field.astype(F32)
    cell = lax.broadcasted_iota(jnp.int32, (chans, cells), 1)
    column = lax.rem(cell, across)
    moved = [
        jnp.where(column == 0, 0.0, pltpu.roll(wide, 1, 1)),
        wide,
        jnp.where(column == across - 1, 0.0, pltpu.roll(wide, cells - 1, 1)),
    ]
    if across % 128 == 0:
        moved = [m.astype(BF16) for m in moved]
        edge = jnp.zeros((chans, across), BF16)
        above = [jnp.concatenate([edge, m[:, :-across]], axis=1) for m in moved]
        below = [jnp.concatenate([m[:, across:], edge], axis=1) for m in moved]
        return above + moved + below
    above = [jnp.where(cell < across, 0.0, pltpu.roll(m, across, 1)) for m in moved]
    below = [
        jnp.where(cell >= cells - across, 0.0, pltpu.roll(m, cells - across, 1)) for m in moved
    ]
    return [m.astype(BF16) for m in above + moved + below]


def kernel(
    n, owners, across,
    feats_hbm, cot_hbm, w1_hbm, w2_hbm,
    out_feats, out_one, out_two,
    feats_in, cot_in, w1, w2, feats, rel, cot, crel, w1f, w1b, w2f, w2b, halo, cots, pools, x1, x2, xg1, xg2, slopes, edges, beyond, shrink, spread,
    part1, land1, full1, part2, land2, full2,
    send_f, recv_f, send_c, recv_c, load, send_p, recv_p, send_e, recv_e,
    send_r1, recv_r1, send_a1, recv_a1, send_r2, recv_r2, send_a2, recv_a2,
):
    place = lax.axis_index("depth")
    core = lax.axis_index("chan")
    other = 1 - core
    half = feats.shape[1]
    cells = feats.shape[2]
    small = cot.shape[1]
    rows1 = 9 * half
    stride = n // owners

    def at(step):
        return lax.rem(place + step + n, n)

    barrier = pltpu.get_barrier_semaphore()

    def greet(device):
        pl.semaphore_signal(barrier, inc=1, device_id=device, device_id_type=MESH)

    greet((place, other))
    for step in (1, -1, 2, -2):
        greet((at(step), other))

    def greet_row(step, carry):
        greet((at(step), core))
        return carry

    lax.fori_loop(1, n, greet_row, 0)

    loads = [
        pltpu.make_async_copy(source, target, load.at[index])
        for index, (source, target) in enumerate(
            ((feats_hbm, feats_in), (cot_hbm, cot_in), (w1_hbm, w1), (w2_hbm, w2))
        )
    ]
    for one in loads:
        one.start()

    def valid(step):
        return jnp.logical_and(place + step >= 0, place + step < n)

    def put_x1(plane, side, field):
        for tap, block in enumerate(plane_taps(field, across)):
            x1[side, pl.ds(plane * rows1 + tap * half, half), :] = block

    rows = cells // across
    loads[0].wait()
    for plane in range(2):
        rel[plane] = feats_in[:, plane].astype(F32).reshape(half * rows, across)
        for row in range(rows):
            feats[plane, :, row * across : (row + 1) * across] = rel[
                plane, pl.ds(row, half, stride=rows), :
            ].astype(BF16)
    loads[1].wait()
    short = small // (across // 2)
    for chan in range(cot.shape[0]):
        crel[chan * 8 : chan * 8 + short, :] = cot_in[chan, 0].astype(F32)
    lines = [crel[pl.ds(row, cot.shape[0], stride=8), :] for row in range(short)]
    cot[...] = jnp.concatenate(lines, axis=1).astype(BF16)
    pl.semaphore_wait(barrier, n + 4)

    def copy(src, dst, send, recv, device):
        return pltpu.make_async_remote_copy(
            src_ref=src, dst_ref=dst, send_sem=send, recv_sem=recv,
            device_id=device, device_id_type=MESH,
        )

    def launch(one, step):
        pl.when(valid(step))(lambda: one.start())

    def arrive(pairs):
        for one, step in pairs:
            pl.when(valid(-step))(lambda one=one: one.wait_recv())

    def leave(pairs):
        for one, step in pairs:
            pl.when(valid(step))(lambda one=one: one.wait_send())

    near = []
    mate = copy(feats, halo.at[pl.ds(1, 2), core], send_f.at[0], recv_f.at[0], (place, other))
    mate.start()
    index = 1
    for step, plane, to in ((1, 1, 0), (-1, 0, 3)):
        for who in (core, other):
            one = copy(
                feats.at[plane], halo.at[to, core], send_f.at[index], recv_f.at[index],
                (at(step), who),
            )
            launch(one, step)
            near.append((one, step))
            index += 1
    cot_copies = []
    index = 0
    targets = [(0, other)] + [(s, w) for s in (1, -1, 2, -2) for w in (core, other)]
    for step, who in targets:
        one = copy(
            cot, cots.at[2 - step, core], send_c.at[index], recv_c.at[index], (at(step), who)
        )
        launch(one, step)
        cot_copies.append((one, step))
        index += 1

    def take_halo(plane, side, keep):
        field = halo[plane, side]
        if keep is not None:
            field = jnp.where(keep, field.astype(F32), 0.0)
        put_x1(plane, side, field)

    def conv_one(plane):
        total = dot(w1f[0], x1[0, (plane - 1) * rows1 : (plane + 2) * rows1, :])
        return total + dot(w1f[1], x1[1, (plane - 1) * rows1 : (plane + 2) * rows1, :])

    cots[2, core] = cot[...]

    for plane in range(2):
        put_x1(1 + plane, core, feats[plane])
    x1[:, 4 * rows1 :, :] = jnp.zeros((2, x1.shape[1] - 4 * rows1, cells), BF16)
    loads[2].wait()
    loads[3].wait()
    taps, mids, _ = w1.shape
    outs = w2.shape[2]
    for side in range(2):
        lo, hi = side * half, (side + 1) * half
        for tap in range(taps):
            w1f[side, :, tap * half : (tap + 1) * half] = w1[tap][:, lo:hi]
        w2f[side] = w2[:, lo:hi, :].reshape(taps * half, outs).T
    w1b[...] = w1[...].reshape(taps * mids, mids).T.reshape(2, half, taps * mids)
    for tap in range(taps):
        w2b[:, tap * outs : (tap + 1) * outs] = w2[tap]
    big_row = lax.broadcasted_iota(jnp.int32, (cells, small), 0)
    small_col = lax.broadcasted_iota(jnp.int32, (cells, small), 1)
    target = (big_row // (2 * across)) * (across // 2) + lax.rem(big_row, across) // 2
    shrink[...] = jnp.where(target == small_col, 0.125, 0.0).astype(BF16)
    big_col = lax.broadcasted_iota(jnp.int32, (small, cells), 1)
    small_row = lax.broadcasted_iota(jnp.int32, (small, cells), 0)
    target = (big_col // (2 * across)) * (across // 2) + lax.rem(big_col, across) // 2
    spread[...] = jnp.where(target == small_row, 0.125, 0.0).astype(BF16)

    mate.wait_recv()
    for plane in (1, 2):
        take_halo(plane, other, None)
    arrive(near)
    for plane, step in ((0, -1), (3, 1)):
        for side in range(2):
            take_halo(plane, side, valid(step))

    pooled = None
    for plane in range(2):
        pre = conv_one(plane + 1)
        sig = jax.nn.sigmoid(pre)
        bend = sig * (1.0 + pre * (1.0 - sig))
        slopes[plane] = bend
        edges[plane] = bend.astype(BF16)
        term = dot((pre * sig).astype(BF16), shrink[...])
        pooled = term if pooled is None else pooled + term
    pools[3] = pooled.astype(BF16)
    pool_copies = []
    for index, step in enumerate((1, -1, 2, -2, 3, -3)):
        one = copy(
            pools.at[3], pools.at[3 - step], send_p.at[index], recv_p.at[index], (at(step), core)
        )
        launch(one, step)
        pool_copies.append((one, step))

    edge_copies = []
    for index, step in enumerate((1, -1)):
        one = copy(
            edges.at[1 - index], beyond.at[index], send_e.at[index], recv_e.at[index],
            (at(step), core),
        )
        launch(one, step)
        edge_copies.append((one, step))

    def put_x2(plane, keep):
        field = pools[plane].astype(F32)
        if keep is not None:
            field = jnp.where(keep, field, 0.0)
        for tap, block in enumerate(plane_taps(field, across // 2)):
            for side in range(2):
                x2[side, pl.ds(plane * rows1 + tap * half, half), :] = block[
                    side * half : (side + 1) * half
                ]

    rows2 = 9 * outs

    def level_two(plane):
        pre = dot(w2f[0], x2[0, plane * rows1 : (plane + 3) * rows1, :])
        pre = pre + dot(w2f[1], x2[1, plane * rows1 : (plane + 3) * rows1, :])
        grad = cots[plane].reshape(outs, small).astype(F32) * slope(pre)
        if plane != 2:
            grad = jnp.where(valid(plane - 2), grad, 0.0)
        return grad.astype(BF16)

    def put_xg2(plane, grad):
        for tap, block in enumerate(plane_taps(grad, across // 2)):
            xg2[pl.ds((4 - plane) * rows2 + (8 - tap) * outs, outs), :] = block

    def back(plane):
        total = dot(w2b[...], xg2[(2 - plane) * rows2 : (5 - plane) * rows2, :])
        return dot(total.astype(BF16), spread[...])

    lanes = 512
    mine = place // stride
    is_owner = lax.rem(place, stride) == 0

    def when_owner(body):
        if stride == 1:
            body()
        else:
            pl.when(is_owner)(body)

    def chunk_out(total, part):
        rows = part.shape[1]
        for chunk in range(owners):
            r, l = chunk // 4, chunk % 4
            part[chunk] = total[r * rows : (r + 1) * rows, l * 128 : (l + 1) * 128].astype(BF16)

    def scatter_copy(part, land, send, recv, chunk, source, device):
        return copy(part.at[chunk], land.at[source], send.at[chunk], recv.at[source], device)

    def scatter(part, land, send, recv):
        def go(step, carry):
            chunk = lax.rem(mine + step, owners)

            @pl.when(chunk * stride != place)
            def _():
                scatter_copy(part, land, send, recv, chunk, place, (chunk * stride, core)).start()

            return carry

        lax.fori_loop(0, owners, go, 0)

        @when_owner
        def _():
            land[place] = part[mine]

    def gather(part, land, full, recv_r, send, recv):
        @when_owner
        def _():
            def arrived(step, carry):
                source = at(step)
                scatter_copy(part, land, send, recv_r, 0, source, (place, other)).wait_recv()
                return carry

            lax.fori_loop(1, n, arrived, 0)
            full[mine] = jnp.sum(land[...].astype(F32), axis=0).astype(BF16)

            def go(step, carry):
                copy(
                    full.at[mine], full.at[mine], send.at[at(step)], recv.at[mine], (at(step), core)
                ).start()
                return carry

            lax.fori_loop(1, n, go, 0)

    def finish(part, land, full, send_r, send, recv, out):
        def came(chunk, carry):
            @pl.when(chunk * stride != place)
            def _():
                copy(
                    full.at[chunk], full.at[chunk], send.at[0], recv.at[chunk], (place, other)
                ).wait_recv()
                scatter_copy(part, land, send_r, recv, chunk, 0, (place, other)).wait_send()

            return carry

        lax.fori_loop(0, owners, came, 0)

        @when_owner
        def _():
            def sent(step, carry):
                copy(
                    full.at[mine], full.at[mine], send.at[at(step)], recv.at[0], (place, other)
                ).wait_send()
                return carry

            lax.fori_loop(1, n, sent, 0)

        out[...] = full[...]

    put_x2(3, None)
    arrive(cot_copies[:1])
    arrive(pool_copies[:2])
    for plane in (2, 4):
        put_x2(plane, valid(plane - 3))
    grad = level_two(2)
    total2 = dot_nt(grad, x2[core, 2 * rows1 : 2 * rows1 + lanes, :])
    chunk_out(total2, part2)
    scatter(part2, land2, send_r2, recv_r2)
    put_xg2(2, grad)

    arrive(cot_copies[1:5])
    arrive(pool_copies[2:4])
    for plane in (1, 5):
        put_x2(plane, valid(plane - 3))
    for plane in (1, 3):
        put_xg2(plane, level_two(plane))

    wide = back(1)
    inner = [(wide * slopes[plane]).astype(BF16) for plane in range(2)]
    total1 = dot_nt(inner[0], x1[core, :lanes, :])
    total1 = total1 + dot_nt(inner[1], x1[core, rows1 : rows1 + lanes, :])
    chunk_out(total1, part1)
    scatter(part1, land1, send_r1, recv_r1)

    arrive(cot_copies[5:])
    arrive(pool_copies[4:])
    for plane in (0, 6):
        put_x2(plane, valid(plane - 3))
    for plane in (0, 4):
        put_xg2(plane, level_two(plane))
    arrive(edge_copies)
    outer = []
    for index, step in enumerate((-1, 1)):
        grad = back(1 + step) * beyond[index].astype(F32)
        outer.append(jnp.where(valid(step), grad, 0.0).astype(BF16))
    grads = [outer[0], inner[0], inner[1], outer[1]]
    gather(part2, land2, full2, recv_r2, send_a2, recv_a2)

    rows_g = 9 * mids
    for plane in range(4):
        for tap, block in enumerate(plane_taps(grads[plane], across)):
            xg1[pl.ds((3 - plane) * rows_g + (8 - tap) * mids, mids), :] = block
    for plane in range(2):
        field = dot(w1b[core], xg1[(1 - plane) * rows_g : (4 - plane) * rows_g, :])
        out_feats[plane] = field.astype(BF16)

    gather(part1, land1, full1, recv_r1, send_a1, recv_a1)
    mate.wait_send()
    leave(near + cot_copies + pool_copies + edge_copies)
    finish(part2, land2, full2, send_r2, send_a2, recv_a2, out_two)
    finish(part1, land1, full1, send_r1, send_a1, recv_a1, out_one)


def layout_kernel(fields, one, two, out_feats, out_one, out_two, rel):
    half, planes, rows, across = out_feats.shape
    for plane in range(planes):
        for row in range(rows):
            rel[plane, pl.ds(row, half, stride=rows), :] = fields[
                plane, :, row * across : (row + 1) * across
            ].astype(F32)
        out_feats[:, plane] = rel[plane].reshape(half, rows, across).astype(BF16)
    for full, out in ((one, out_one), (two, out_two)):
        bands = [
            jnp.concatenate([full[4 * r + l].astype(F32) for l in range(4)], axis=1)
            for r in range(full.shape[0] // 4)
        ]
        out[...] = jnp.concatenate(bands, axis=0).T[: out.shape[0]]


def shards(feats, weight_one, weight_two, cotangent):
    n = lax.axis_size("depth")
    owners = 16
    half, planes, height, across = feats.shape
    cells = height * across
    mids = weight_one.shape[0]
    outs = weight_two.shape[0]
    small = cells // 4
    taps = weight_one.shape[2]
    w1 = jnp.transpose(weight_one, (2, 0, 1))
    w2 = jnp.transpose(weight_two, (2, 1, 0))
    vmem = pl.BlockSpec(memory_space=pltpu.VMEM)
    dma = pltpu.SemaphoreType.DMA
    packed = pl.pallas_call(
        functools.partial(kernel, n, owners, across),
        out_shape=(
            jax.ShapeDtypeStruct((planes, half, cells), BF16),
            jax.ShapeDtypeStruct((owners, mids // 4, 128), BF16),
            jax.ShapeDtypeStruct((owners, outs // 4, 128), BF16),
        ),
        in_specs=[pl.BlockSpec(memory_space=pltpu.HBM)] * 4,
        out_specs=(vmem,) * 3,
        scratch_shapes=[
            pltpu.VMEM(feats.shape, BF16),
            pltpu.VMEM(cotangent.shape, BF16),
            pltpu.VMEM(w1.shape, BF16),
            pltpu.VMEM(w2.shape, BF16),
            pltpu.VMEM((planes, half, cells), BF16),
            pltpu.VMEM((planes, half * height, across), F32),
            pltpu.VMEM((outs // 2, small), BF16),
            pltpu.VMEM((outs // 2 * 8, across // 2), F32),
            pltpu.VMEM((2, mids, taps * half), BF16),
            pltpu.VMEM((2, half, taps * mids), BF16),
            pltpu.VMEM((2, outs, taps * half), BF16),
            pltpu.VMEM((mids, taps * outs), BF16),
            pltpu.VMEM((4, 2, half, cells), BF16),
            pltpu.VMEM((5, 2, outs // 2, small), BF16),
            pltpu.VMEM((7, mids, small), BF16),
            pltpu.VMEM((2, 5 * 9 * half, cells), BF16),
            pltpu.VMEM((2, 7 * 9 * half, small), BF16),
            pltpu.VMEM((4 * 9 * mids, cells), BF16),
            pltpu.VMEM((5 * 9 * outs, small), BF16),
            pltpu.VMEM((2, mids, cells), F32),
            pltpu.VMEM((2, mids, cells), BF16),
            pltpu.VMEM((2, mids, cells), BF16),
            pltpu.VMEM((cells, small), BF16),
            pltpu.VMEM((small, cells), BF16),
            pltpu.VMEM((owners, mids // 4, 128), BF16),
            pltpu.VMEM((n, mids // 4, 128), BF16),
            pltpu.VMEM((owners, mids // 4, 128), BF16),
            pltpu.VMEM((owners, outs // 4, 128), BF16),
            pltpu.VMEM((n, outs // 4, 128), BF16),
            pltpu.VMEM((owners, outs // 4, 128), BF16),
            dma((5,)), dma((5,)), dma((9,)), dma((9,)), dma((4,)), dma((6,)), dma((6,)), dma((2,)), dma((2,)),
            dma((owners,)), dma((n,)), dma((n,)), dma((owners,)),
            dma((owners,)), dma((n,)), dma((n,)), dma((owners,)),
        ],
        compiler_params=pltpu.CompilerParams(
            collective_id=0, has_side_effects=True, vmem_limit_bytes=28 * 1024 * 1024
        ),
    )(feats, cotangent, w1, w2)

    out_feats, out_one, out_two = pl.pallas_call(
        layout_kernel,
        out_shape=(
            jax.ShapeDtypeStruct(feats.shape, BF16),
            jax.ShapeDtypeStruct((taps * half, mids), F32),
            jax.ShapeDtypeStruct((taps * half, outs), F32),
        ),
        in_specs=[vmem] * 3,
        out_specs=(vmem,) * 3,
        scratch_shapes=[pltpu.VMEM((planes, half * height, across), F32)],
        compiler_params=pltpu.CompilerParams(vmem_limit_bytes=8 * 1024 * 1024),
    )(*packed)

    def layout(total):
        return jnp.transpose(total.reshape(taps, half, total.shape[1]), (2, 1, 0))

    return out_feats, layout(out_one), layout(out_two)


def solution(mesh):
    return jax.shard_map(
        shards,
        mesh=mesh,
        in_specs=(P("chan", "depth", None, None), P(), P(), P("chan", "depth", None, None)),
        out_specs=(P("chan", "depth", None, None), P(None, "chan", None), P(None, "chan", None)),
        check_vma=False,
    )
```

```python
import functools

import jax
import jax.numpy as jnp
from jax import lax
from jax.experimental import pallas as pl
from jax.experimental.pallas import tpu as pltpu
from jax.sharding import PartitionSpec as P

MESH = pl.DeviceIdType.MESH
BF16 = jnp.bfloat16
F32 = jnp.float32


def dot(left, right):
    return jnp.dot(left, right, preferred_element_type=F32)


def dot_nt(left, right):
    return lax.dot_general(left, right, (((1,), (1,)), ((), ())), preferred_element_type=F32)


def slope(pre):
    sig = jax.nn.sigmoid(pre)
    return sig * (1.0 + pre * (1.0 - sig))


def plane_taps(field, across):
    chans, cells = field.shape
    wide = field.astype(F32)
    cell = lax.broadcasted_iota(jnp.int32, (chans, cells), 1)
    column = lax.rem(cell, across)
    moved = [
        jnp.where(column == 0, 0.0, pltpu.roll(wide, 1, 1)),
        wide,
        jnp.where(column == across - 1, 0.0, pltpu.roll(wide, cells - 1, 1)),
    ]
    if across % 128 == 0:
        moved = [m.astype(BF16) for m in moved]
        edge = jnp.zeros((chans, across), BF16)
        above = [jnp.concatenate([edge, m[:, :-across]], axis=1) for m in moved]
        below = [jnp.concatenate([m[:, across:], edge], axis=1) for m in moved]
        return above + moved + below
    above = [jnp.where(cell < across, 0.0, pltpu.roll(m, across, 1)) for m in moved]
    below = [
        jnp.where(cell >= cells - across, 0.0, pltpu.roll(m, cells - across, 1)) for m in moved
    ]
    return [m.astype(BF16) for m in above + moved + below]


def kernel(
    n, owners, across,
    feats_hbm, cot_hbm, w1_hbm, w2_hbm,
    out_feats, out_one, out_two,
    feats_in, cot_in, w1, w2, feats, rel, cot, crel, w1f, w1b, w2f, w2b, halo, cots, pools, x1, x2, xg1, xg2, slopes, edges, beyond, shrink, spread,
    part1, land1, full1, part2, land2, full2,
    send_f, recv_f, send_c, recv_c, load, send_p, recv_p, send_e, recv_e,
    send_r1, recv_r1, send_a1, recv_a1, send_r2, recv_r2, send_a2, recv_a2,
):
    place = lax.axis_index("depth")
    core = lax.axis_index("chan")
    other = 1 - core
    half = feats.shape[1]
    cells = feats.shape[2]
    small = cot.shape[1]
    rows1 = 9 * half
    stride = n // owners

    def at(step):
        return lax.rem(place + step + n, n)

    barrier = pltpu.get_barrier_semaphore()

    def greet(device):
        pl.semaphore_signal(barrier, inc=1, device_id=device, device_id_type=MESH)

    greet((place, other))
    for step in (1, -1, 2, -2):
        greet((at(step), other))

    def greet_row(step, carry):
        greet((at(step), core))
        return carry

    lax.fori_loop(1, n, greet_row, 0)

    loads = [
        pltpu.make_async_copy(source, target, load.at[index])
        for index, (source, target) in enumerate(
            ((feats_hbm, feats_in), (cot_hbm, cot_in), (w1_hbm, w1), (w2_hbm, w2))
        )
    ]
    for one in loads:
        one.start()

    def valid(step):
        return jnp.logical_and(place + step >= 0, place + step < n)

    def put_x1(plane, side, field):
        for tap, block in enumerate(plane_taps(field, across)):
            x1[side, pl.ds(plane * rows1 + tap * half, half), :] = block

    rows = cells // across
    loads[0].wait()
    for plane in range(2):
        rel[plane] = feats_in[:, plane].astype(F32).reshape(half * rows, across)
        for row in range(rows):
            feats[plane, :, row * across : (row + 1) * across] = rel[
                plane, pl.ds(row, half, stride=rows), :
            ].astype(BF16)
    loads[1].wait()
    short = small // (across // 2)
    for chan in range(cot.shape[0]):
        crel[chan * 8 : chan * 8 + short, :] = cot_in[chan, 0].astype(F32)
    lines = [crel[pl.ds(row, cot.shape[0], stride=8), :] for row in range(short)]
    cot[...] = jnp.concatenate(lines, axis=1).astype(BF16)
    pl.semaphore_wait(barrier, n + 4)

    def copy(src, dst, send, recv, device):
        return pltpu.make_async_remote_copy(
            src_ref=src, dst_ref=dst, send_sem=send, recv_sem=recv,
            device_id=device, device_id_type=MESH,
        )

    def launch(one, step):
        pl.when(valid(step))(lambda: one.start())

    def arrive(pairs):
        for one, step in pairs:
            pl.when(valid(-step))(lambda one=one: one.wait_recv())

    def leave(pairs):
        for one, step in pairs:
            pl.when(valid(step))(lambda one=one: one.wait_send())

    near = []
    mate = copy(feats, halo.at[pl.ds(1, 2), core], send_f.at[0], recv_f.at[0], (place, other))
    mate.start()
    index = 1
    for step, plane, to in ((1, 1, 0), (-1, 0, 3)):
        for who in (core, other):
            one = copy(
                feats.at[plane], halo.at[to, core], send_f.at[index], recv_f.at[index],
                (at(step), who),
            )
            launch(one, step)
            near.append((one, step))
            index += 1
    cot_copies = []
    index = 0
    targets = [(0, other)] + [(s, w) for s in (1, -1, 2, -2) for w in (core, other)]
    for step, who in targets:
        one = copy(
            cot, cots.at[2 - step, core], send_c.at[index], recv_c.at[index], (at(step), who)
        )
        launch(one, step)
        cot_copies.append((one, step))
        index += 1

    def take_halo(plane, side, keep):
        field = halo[plane, side]
        if keep is not None:
            field = jnp.where(keep, field.astype(F32), 0.0)
        put_x1(plane, side, field)

    def conv_one(plane):
        total = dot(w1f[0], x1[0, (plane - 1) * rows1 : (plane + 2) * rows1, :])
        return total + dot(w1f[1], x1[1, (plane - 1) * rows1 : (plane + 2) * rows1, :])

    cots[2, core] = cot[...]

    for plane in range(2):
        put_x1(1 + plane, core, feats[plane])
    x1[:, 4 * rows1 :, :] = jnp.zeros((2, x1.shape[1] - 4 * rows1, cells), BF16)
    loads[2].wait()
    loads[3].wait()
    taps, mids, _ = w1.shape
    outs = w2.shape[2]
    for side in range(2):
        lo, hi = side * half, (side + 1) * half
        for tap in range(taps):
            w1f[side, :, tap * half : (tap + 1) * half] = w1[tap][:, lo:hi]
        w2f[side] = w2[:, lo:hi, :].reshape(taps * half, outs).T
    w1b[...] = w1[...].reshape(taps * mids, mids).T.reshape(2, half, taps * mids)
    for tap in range(taps):
        w2b[:, tap * outs : (tap + 1) * outs] = w2[tap]
    big_row = lax.broadcasted_iota(jnp.int32, (cells, small), 0)
    small_col = lax.broadcasted_iota(jnp.int32, (cells, small), 1)
    target = (big_row // (2 * across)) * (across // 2) + lax.rem(big_row, across) // 2
    shrink[...] = jnp.where(target == small_col, 0.125, 0.0).astype(BF16)
    big_col = lax.broadcasted_iota(jnp.int32, (small, cells), 1)
    small_row = lax.broadcasted_iota(jnp.int32, (small, cells), 0)
    target = (big_col // (2 * across)) * (across // 2) + lax.rem(big_col, across) // 2
    spread[...] = jnp.where(target == small_row, 0.125, 0.0).astype(BF16)

    mate.wait_recv()
    for plane in (1, 2):
        take_halo(plane, other, None)
    arrive(near)
    for plane, step in ((0, -1), (3, 1)):
        for side in range(2):
            take_halo(plane, side, valid(step))

    pooled = None
    for plane in range(2):
        pre = conv_one(plane + 1)
        sig = jax.nn.sigmoid(pre)
        bend = sig * (1.0 + pre * (1.0 - sig))
        slopes[plane] = bend
        edges[plane] = bend.astype(BF16)
        term = dot((pre * sig).astype(BF16), shrink[...])
        pooled = term if pooled is None else pooled + term
    pools[3] = pooled.astype(BF16)
    pool_copies = []
    for index, step in enumerate((1, -1, 2, -2, 3, -3)):
        one = copy(
            pools.at[3], pools.at[3 - step], send_p.at[index], recv_p.at[index], (at(step), core)
        )
        launch(one, step)
        pool_copies.append((one, step))

    edge_copies = []
    for index, step in enumerate((1, -1)):
        one = copy(
            edges.at[1 - index], beyond.at[index], send_e.at[index], recv_e.at[index],
            (at(step), core),
        )
        launch(one, step)
        edge_copies.append((one, step))

    def put_x2(plane, keep):
        field = pools[plane].astype(F32)
        if keep is not None:
            field = jnp.where(keep, field, 0.0)
        for tap, block in enumerate(plane_taps(field, across // 2)):
            for side in range(2):
                x2[side, pl.ds(plane * rows1 + tap * half, half), :] = block[
                    side * half : (side + 1) * half
                ]

    rows2 = 9 * outs

    def level_two(plane):
        pre = dot(w2f[0], x2[0, plane * rows1 : (plane + 3) * rows1, :])
        pre = pre + dot(w2f[1], x2[1, plane * rows1 : (plane + 3) * rows1, :])
        grad = cots[plane].reshape(outs, small).astype(F32) * slope(pre)
        if plane != 2:
            grad = jnp.where(valid(plane - 2), grad, 0.0)
        return grad.astype(BF16)

    def put_xg2(plane, grad):
        for tap, block in enumerate(plane_taps(grad, across // 2)):
            xg2[pl.ds((4 - plane) * rows2 + (8 - tap) * outs, outs), :] = block

    def back(plane):
        total = dot(w2b[...], xg2[(2 - plane) * rows2 : (5 - plane) * rows2, :])
        return dot(total.astype(BF16), spread[...])

    lanes = 512
    mine = place // stride
    is_owner = lax.rem(place, stride) == 0

    def when_owner(body):
        if stride == 1:
            body()
        else:
            pl.when(is_owner)(body)

    def chunk_out(total, part):
        rows = part.shape[1]
        for chunk in range(owners):
            r, l = chunk // 4, chunk % 4
            part[chunk] = total[r * rows : (r + 1) * rows, l * 128 : (l + 1) * 128].astype(BF16)

    def scatter_copy(part, land, send, recv, chunk, source, device):
        return copy(part.at[chunk], land.at[source], send.at[chunk], recv.at[source], device)

    def scatter(part, land, send, recv):
        def go(step, carry):
            chunk = lax.rem(mine + step, owners)

            @pl.when(chunk * stride != place)
            def _():
                scatter_copy(part, land, send, recv, chunk, place, (chunk * stride, core)).start()

            return carry

        lax.fori_loop(0, owners, go, 0)

        @when_owner
        def _():
            land[place] = part[mine]

    def gather(part, land, full, recv_r, send, recv):
        @when_owner
        def _():
            def arrived(step, carry):
                source = at(step)
                scatter_copy(part, land, send, recv_r, 0, source, (place, other)).wait_recv()
                return carry

            lax.fori_loop(1, n, arrived, 0)
            full[mine] = jnp.sum(land[...].astype(F32), axis=0).astype(BF16)

            def go(step, carry):
                copy(
                    full.at[mine], full.at[mine], send.at[at(step)], recv.at[mine], (at(step), core)
                ).start()
                return carry

            lax.fori_loop(1, n, go, 0)

    def finish(part, land, full, send_r, send, recv, out):
        def came(chunk, carry):
            @pl.when(chunk * stride != place)
            def _():
                copy(
                    full.at[chunk], full.at[chunk], send.at[0], recv.at[chunk], (place, other)
                ).wait_recv()
                scatter_copy(part, land, send_r, recv, chunk, 0, (place, other)).wait_send()

            return carry

        lax.fori_loop(0, owners, came, 0)

        @when_owner
        def _():
            def sent(step, carry):
                copy(
                    full.at[mine], full.at[mine], send.at[at(step)], recv.at[0], (place, other)
                ).wait_send()
                return carry

            lax.fori_loop(1, n, sent, 0)

        out[...] = full[...]

    put_x2(3, None)
    arrive(cot_copies[:1])
    arrive(pool_copies[:2])
    for plane in (2, 4):
        put_x2(plane, valid(plane - 3))
    grad = level_two(2)
    total2 = dot_nt(grad, x2[core, 2 * rows1 : 2 * rows1 + lanes, :])
    chunk_out(total2, part2)
    scatter(part2, land2, send_r2, recv_r2)
    put_xg2(2, grad)

    arrive(cot_copies[1:5])
    arrive(pool_copies[2:4])
    for plane in (1, 5):
        put_x2(plane, valid(plane - 3))
    for plane in (1, 3):
        put_xg2(plane, level_two(plane))

    wide = back(1)
    inner = [(wide * slopes[plane]).astype(BF16) for plane in range(2)]
    total1 = dot_nt(inner[0], x1[core, :lanes, :])
    total1 = total1 + dot_nt(inner[1], x1[core, rows1 : rows1 + lanes, :])
    chunk_out(total1, part1)
    scatter(part1, land1, send_r1, recv_r1)

    arrive(cot_copies[5:])
    arrive(pool_copies[4:])
    for plane in (0, 6):
        put_x2(plane, valid(plane - 3))
    for plane in (0, 4):
        put_xg2(plane, level_two(plane))
    arrive(edge_copies)
    outer = []
    for index, step in enumerate((-1, 1)):
        grad = back(1 + step) * beyond[index].astype(F32)
        outer.append(jnp.where(valid(step), grad, 0.0).astype(BF16))
    grads = [outer[0], inner[0], inner[1], outer[1]]
    gather(part2, land2, full2, recv_r2, send_a2, recv_a2)

    rows_g = 9 * mids
    for plane in range(4):
        for tap, block in enumerate(plane_taps(grads[plane], across)):
            xg1[pl.ds((3 - plane) * rows_g + (8 - tap) * mids, mids), :] = block
    for plane in range(2):
        field = dot(w1b[core], xg1[(1 - plane) * rows_g : (4 - plane) * rows_g, :])
        out_feats[plane] = field.astype(BF16)

    gather(part1, land1, full1, recv_r1, send_a1, recv_a1)
    mate.wait_send()
    leave(near + cot_copies + pool_copies + edge_copies)
    finish(part2, land2, full2, send_r2, send_a2, recv_a2, out_two)
    finish(part1, land1, full1, send_r1, send_a1, recv_a1, out_one)


def layout_kernel(fields, one, two, out_feats, out_one, out_two, rel):
    half, planes, rows, across = out_feats.shape
    for plane in range(planes):
        for row in range(rows):
            rel[plane, pl.ds(row, half, stride=rows), :] = fields[
                plane, :, row * across : (row + 1) * across
            ].astype(F32)
        out_feats[:, plane] = rel[plane].reshape(half, rows, across).astype(BF16)
    for full, out in ((one, out_one), (two, out_two)):
        bands = [
            jnp.concatenate([full[4 * r + l].astype(F32) for l in range(4)], axis=1)
            for r in range(full.shape[0] // 4)
        ]
        out[...] = jnp.concatenate(bands, axis=0).T[: out.shape[0]]


def shards(feats, weight_one, weight_two, cotangent):
    n = lax.axis_size("depth")
    owners = 16
    half, planes, height, across = feats.shape
    cells = height * across
    mids = weight_one.shape[0]
    outs = weight_two.shape[0]
    small = cells // 4
    taps = weight_one.shape[2]
    w1 = jnp.transpose(weight_one, (2, 0, 1))
    w2 = jnp.transpose(weight_two, (2, 1, 0))
    vmem = pl.BlockSpec(memory_space=pltpu.VMEM)
    dma = pltpu.SemaphoreType.DMA
    packed = pl.pallas_call(
        functools.partial(kernel, n, owners, across),
        out_shape=(
            jax.ShapeDtypeStruct((planes, half, cells), BF16),
            jax.ShapeDtypeStruct((owners, mids // 4, 128), BF16),
            jax.ShapeDtypeStruct((owners, outs // 4, 128), BF16),
        ),
        in_specs=[pl.BlockSpec(memory_space=pl.ANY)] * 4,
        out_specs=(vmem,) * 3,
        scratch_shapes=[
            pltpu.VMEM(feats.shape, BF16),
            pltpu.VMEM(cotangent.shape, BF16),
            pltpu.VMEM(w1.shape, BF16),
            pltpu.VMEM(w2.shape, BF16),
            pltpu.VMEM((planes, half, cells), BF16),
            pltpu.VMEM((planes, half * height, across), F32),
            pltpu.VMEM((outs // 2, small), BF16),
            pltpu.VMEM((outs // 2 * 8, across // 2), F32),
            pltpu.VMEM((2, mids, taps * half), BF16),
            pltpu.VMEM((2, half, taps * mids), BF16),
            pltpu.VMEM((2, outs, taps * half), BF16),
            pltpu.VMEM((mids, taps * outs), BF16),
            pltpu.VMEM((4, 2, half, cells), BF16),
            pltpu.VMEM((5, 2, outs // 2, small), BF16),
            pltpu.VMEM((7, mids, small), BF16),
            pltpu.VMEM((2, 5 * 9 * half, cells), BF16),
            pltpu.VMEM((2, 7 * 9 * half, small), BF16),
            pltpu.VMEM((4 * 9 * mids, cells), BF16),
            pltpu.VMEM((5 * 9 * outs, small), BF16),
            pltpu.VMEM((2, mids, cells), F32),
            pltpu.VMEM((2, mids, cells), BF16),
            pltpu.VMEM((2, mids, cells), BF16),
            pltpu.VMEM((cells, small), BF16),
            pltpu.VMEM((small, cells), BF16),
            pltpu.VMEM((owners, mids // 4, 128), BF16),
            pltpu.VMEM((n, mids // 4, 128), BF16),
            pltpu.VMEM((owners, mids // 4, 128), BF16),
            pltpu.VMEM((owners, outs // 4, 128), BF16),
            pltpu.VMEM((n, outs // 4, 128), BF16),
            pltpu.VMEM((owners, outs // 4, 128), BF16),
            dma((5,)), dma((5,)), dma((9,)), dma((9,)), dma((4,)), dma((6,)), dma((6,)), dma((2,)), dma((2,)),
            dma((owners,)), dma((n,)), dma((n,)), dma((owners,)),
            dma((owners,)), dma((n,)), dma((n,)), dma((owners,)),
        ],
        compiler_params=pltpu.CompilerParams(
            collective_id=0, has_side_effects=True, vmem_limit_bytes=60 * 1024 * 1024
        ),
    )(feats, cotangent, w1, w2)

    out_feats, out_one, out_two = pl.pallas_call(
        layout_kernel,
        out_shape=(
            jax.ShapeDtypeStruct(feats.shape, BF16),
            jax.ShapeDtypeStruct((taps * half, mids), F32),
            jax.ShapeDtypeStruct((taps * half, outs), F32),
        ),
        in_specs=[vmem] * 3,
        out_specs=(vmem,) * 3,
        scratch_shapes=[pltpu.VMEM((planes, half * height, across), F32)],
        compiler_params=pltpu.CompilerParams(vmem_limit_bytes=60 * 1024 * 1024),
    )(*packed)

    def layout(total):
        return jnp.transpose(total.reshape(taps, half, total.shape[1]), (2, 1, 0))

    return out_feats, layout(out_one), layout(out_two)


def solution(mesh):
    return jax.shard_map(
        shards,
        mesh=mesh,
        in_specs=(P("chan", "depth", None, None), P(), P(), P("chan", "depth", None, None)),
        out_specs=(P("chan", "depth", None, None), P(None, "chan", None), P(None, "chan", None)),
        check_vma=False,
    )
```
